256 devices in a mesh: gx: 4 (over z_lo), gy: 16 (over z_hi, y, core), gz: 4 (over x).
Axes of the slice: x: 4, y: 4, z: 8 (z_hi: 2, z_lo: 4; z = z_hi * 4 + z_lo), core: 2. Of those that a mesh axis runs over, the one named last changes fastest.
Arguments:
- positions: float32 [3, 1048576], P(None, ('gx', 'gy', 'gz'))
- velocities: float32 [3, 1048576], P(None, ('gx', 'gy', 'gz')), may hold values from -6 to 6
- forces_old: float32 [3, 1048576], P(None, ('gx', 'gy', 'gz')), may hold values from -6 to 6
- inv_mass: float32 [1048576], P(('gx', 'gy', 'gz')), may hold values from 0.25 to 4
- charges: float32 [1048576], P(('gx', 'gy', 'gz')), may hold values from -3 to 3
- block_species: int32 [8192], P(('gx', 'gy', 'gz')), may hold values from 0 to 3
- sigma_table: float32 [4], replicated, may hold values from 0.25 to 0.5
- epsilon_table: float32 [4], replicated, may hold values from 0.02 to 0.2
- tower_index: int32 [256, 64], P(('gx', 'gy', 'gz')), may hold values from 0 to 127
- plate_index: int32 [256, 64], P(('gx', 'gy', 'gz')), may hold values from 0 to 287
- tile_counts: int32 [256], P(('gx', 'gy', 'gz')), may hold values from 1 to 64, as said below
- exclusions: int32 [256, 64, 16, 128], P(('gx', 'gy', 'gz')), may hold values from 0 to 255, as said below
- mig_block: int32 [256, 4], P(('gx', 'gy', 'gz')), may hold values from 0 to 31, as said below
- mig_dest: int32 [256, 4], P(('gx', 'gy', 'gz')), may hold values from 0 to 8, as said below
Outputs:
- positions_new: float32 [3, 1048576], P(None, ('gx', 'gy', 'gz'))
- velocities_new: float32 [3, 1048576], P(None, ('gx', 'gy', 'gz'))
- forces_new: float32 [3, 1048576], P(None, ('gx', 'gy', 'gz'))
- arrivals: float32 [6, 256, 8, 512], P(None, ('gx', 'gy', 'gz'))
The draws below stay inside these ranges and needn't reach their ends.
Inputs may be any that keep to these rules, and one draw needn't show every extreme that they name: `tile_counts`: at most 64 for every box, and exactly 64 for some box; slots at or after a box's count carry no weight. `exclusions`: each of the low eight bits marks one excluded atom pair. `mig_block`: the 4 entries of one box are distinct. `mig_dest`: never 4.
All inputs are finite; a program needn't handle non-finite values.
Results may differ from the reference program's by a relative error of at most 0.0003.
Values sent between devices are 32-bit elements; how exact they have to be, the bound alone decides.
No kernel may reach another device: no remote copies, remote signals or barrier semaphores. Data moves between devices by JAX's collectives and lax.ppermute only.
A program may use at most 64 MiB of HBM per device.

```python
import math
import jax
import jax.numpy as jnp
from jax import lax

TILE = 128
WORDS = 16
BLOCKS = 32
PAIRS = 64
MIG = 4
KINDS = 4
ATOMS = 1048576
N_GX = 4
N_GY = 16
N_GZ = 4
DEVICES = 256


def draw_positions(key, part):
    atoms_box = BLOCKS * TILE
    atom_ids = jnp.arange(atoms_box * DEVICES, dtype=jnp.int32)
    box_ids = atom_ids // atoms_box
    coord_x = (box_ids // (N_GY * N_GZ)).astype(jnp.float32)
    coord_y = (box_ids // N_GZ % N_GY).astype(jnp.float32)
    coord_z = (box_ids % N_GZ).astype(jnp.float32)
    spread = jax.random.uniform(key, (3, atoms_box * DEVICES), jnp.float32)
    layer_height = 1.0 / N_GZ
    return jnp.stack([coord_x + spread[0], coord_y + spread[1], (coord_z + spread[2]) * layer_height], axis=0).astype(jnp.float32)


def draw_tile_counts(key, part):
    first_key, second_key, third_key = jax.random.split(jax.random.fold_in(key, 11), 3)
    left = jax.random.randint(first_key, (DEVICES,), 1, PAIRS + 1)
    right = jax.random.randint(second_key, (DEVICES,), 1, PAIRS + 1)
    counted = jnp.maximum(left * right // PAIRS, 1)
    busiest = jax.random.randint(third_key, (), 0, DEVICES)
    counted = jnp.where(jnp.arange(DEVICES) == busiest, PAIRS, counted)
    return counted.astype(jnp.int32)


def draw_exclusions(key, part):
    first_key, second_key = jax.random.split(jax.random.fold_in(key, 23), 2)
    shape_full = (DEVICES, PAIRS, WORDS, TILE)
    first_bits = jax.random.randint(first_key, shape_full, 0, 256, dtype=jnp.int32)
    second_bits = jax.random.randint(second_key, shape_full, 0, 256, dtype=jnp.int32)
    return jnp.bitwise_and(first_bits, second_bits).astype(jnp.int32)


def draw_mig_block(key, part):
    row_keys = jax.random.split(jax.random.fold_in(key, 37), DEVICES)
    orders = jax.vmap(lambda row_key: jax.random.permutation(row_key, BLOCKS))(row_keys)
    return orders[:, :MIG].astype(jnp.int32)


def draw_mig_dest(key, part):
    picked = jax.random.randint(jax.random.fold_in(key, 41), (DEVICES, MIG), 0, 8)
    return (picked + (picked >= 4).astype(picked.dtype)).astype(jnp.int32)


def plant(values, own_key, least, high):
    dims = values.shape
    place = [jax.random.randint(jax.random.fold_in(own_key, axis), (), 0, dims[axis]) for axis in range(len(dims))]
    values = values.at[tuple(place)].set(least)
    longest = dims.index(max(dims))
    place[longest] = (place[longest] + 1) % dims[longest]
    return values.at[tuple(place)].set(high)


def steps_of(rng, extent, cuts, least, top_value):
    factor_of = 1.0
    for position, blocks in cuts:
        heights = jax.random.uniform(jax.random.fold_in(jax.random.fold_in(rng, 6), position), (blocks,), jnp.float32, least / len(cuts), top_value / len(cuts))
        factor_of = factor_of * jnp.repeat(jnp.exp(heights), extent[position] // blocks).reshape((-1,) + (1,) * (len(extent) - 1 - position))
    return factor_of


def normal_values(key, dims, scale, reach, shards=(), kind=jnp.bfloat16):
    drawn = jax.random.normal(key, dims, jnp.float32) * scale
    if len(shards) > 0:
        drawn = steps_of(key, dims, shards, -0.22, 0.18) * drawn
    return jnp.clip(drawn, min=-reach, max=reach).astype(kind)


def setup_inputs(seed: int = 0) -> dict:
    splits = jax.random.split(jax.random.key(seed), 15)
    return {
        "positions": draw_positions(jax.random.fold_in(splits[14], 71), 0),
        "velocities": normal_values(splits[1], (3, ATOMS), 1.0, 6.0, ((1, 256),), jnp.float32),
        "forces_old": normal_values(splits[2], (3, ATOMS), 1.0, 6.0, ((1, 256),), jnp.float32),
        "inv_mass": jnp.clip(jnp.exp(math.log(4.0) - 2.7725887 * jax.random.uniform(splits[3], (ATOMS,), jnp.float32) ** steps_of(splits[3], (ATOMS,), ((0, 256),), -0.2, 0.2)), 0.25, 4.0),
        "charges": normal_values(splits[4], (ATOMS,), 0.5, 3.0, ((0, 256),), jnp.float32),
        "block_species": plant(jax.random.randint(splits[5], (DEVICES * BLOCKS,), 0, KINDS), jax.random.fold_in(splits[5], 1), 0, KINDS - 1).astype(jnp.int32),
        "sigma_table": jnp.clip(jnp.exp(jax.random.uniform(splits[6], (KINDS,), jnp.float32, math.log(0.25), math.log(0.5))), 0.25, 0.5),
        "epsilon_table": jnp.clip(jnp.exp(jax.random.uniform(splits[7], (KINDS,), jnp.float32, math.log(0.02), math.log(0.2))), 0.02, 0.2),
        "tower_index": plant(jax.random.randint(splits[8], (DEVICES, PAIRS), 0, N_GZ * BLOCKS), jax.random.fold_in(splits[8], 1), 0, (N_GZ * BLOCKS) - 1).astype(jnp.int32),
        "plate_index": plant(jax.random.randint(splits[9], (DEVICES, PAIRS), 0, 9 * BLOCKS), jax.random.fold_in(splits[9], 1), 0, (9 * BLOCKS) - 1).astype(jnp.int32),
        "tile_counts": draw_tile_counts(jax.random.fold_in(splits[14], 71), 0),
        "exclusions": draw_exclusions(jax.random.fold_in(splits[14], 71), 0),
        "mig_block": draw_mig_block(jax.random.fold_in(splits[14], 71), 0),
        "mig_dest": draw_mig_dest(jax.random.fold_in(splits[14], 71), 0),
    }


time_step = 0.2
soft_core = 0.09
cutoff_sq = 1.44
coulomb_k = 0.5

def tile_terms(tower_rows, plate_rows, mask_words, length_x, length_y):
    tile_width = tower_rows.shape[1]
    raw = tower_rows[0:3, :, None] - plate_rows[0:3, None, :]
    image_x = raw[0] - length_x * jnp.floor(raw[0] / length_x + 0.5)
    image_y = raw[1] - length_y * jnp.floor(raw[1] / length_y + 0.5)
    offsets = jnp.stack([image_x, image_y, raw[2]], axis=0)
    distance_sq = lax.optimization_barrier(jnp.sum(offsets * offsets, axis=0))
    inverse = 1.0 / (distance_sq + soft_core)
    sigma_pair = 0.5 * (tower_rows[4][:, None] + plate_rows[4][None, :])
    ratio_pair = sigma_pair * sigma_pair * inverse
    ratio_cube = ratio_pair * ratio_pair * ratio_pair
    depth_pair = tower_rows[5][:, None] * plate_rows[5][None, :]
    charge_term = coulomb_k * tower_rows[3][:, None] * plate_rows[3][None, :] * jnp.sqrt(inverse)
    falloff = 1.0 - distance_sq / cutoff_sq
    switch = jnp.where(distance_sq < cutoff_sq, falloff * falloff, 0.0)
    spread = jnp.repeat(mask_words.T, 8, axis=1)
    shifts = jnp.arange(tile_width, dtype=jnp.int32) % 8
    excluded = jnp.bitwise_and(jnp.right_shift(spread, shifts[None, :]), 1)
    kept_pairs = (1 - excluded).astype(jnp.float32)
    strength = (depth_pair * (12.0 * ratio_cube * ratio_cube - 6.0 * ratio_cube) + charge_term) * inverse * switch * kept_pairs
    weighted = strength[None] * offsets
    return (lax.optimization_barrier(jnp.sum(weighted, axis=2)), -lax.optimization_barrier(jnp.sum(weighted, axis=1)))

def box_number(coord_x, coord_y, coord_z):
    return (coord_x * N_GY + coord_y) * N_GZ + coord_z

def reference(positions, velocities, forces_old, inv_mass, charges, block_species, sigma_table, epsilon_table, tower_index, plate_index, tile_counts, exclusions, mig_block, mig_dest):
    half_kick = velocities + 0.5 * time_step * forces_old * inv_mass[None, :]
    moved = positions + time_step * half_kick
    sigma_atom = jnp.repeat(sigma_table[block_species], TILE)
    depth_atom = jnp.repeat(jnp.sqrt(epsilon_table)[block_species], TILE)
    features = jnp.concatenate([moved, charges[None, :], sigma_atom[None, :], depth_atom[None, :]], axis=0)
    block_rows = features.reshape(6, DEVICES * BLOCKS, TILE)
    pair_slots = jnp.arange(PAIRS, dtype=jnp.int32)
    length_x = float(N_GX)
    length_y = float(N_GY)

    def pair_terms(tower_rows, plate_rows, mask_words):
        return tile_terms(tower_rows, plate_rows, mask_words, length_x, length_y)

    def one_box(totals, inputs):
        box_index, tower_list, plate_list, pair_count, mask_list = inputs
        coord_x = box_index // (N_GY * N_GZ)
        coord_y = box_index // N_GZ % N_GY
        coord_z = box_index % N_GZ
        tower_ids = box_number(coord_x, coord_y, tower_list // BLOCKS) * BLOCKS + tower_list % BLOCKS
        neighbour = plate_list // BLOCKS
        plate_ids = box_number((coord_x + neighbour // 3 - 1) % N_GX, (coord_y + neighbour % 3 - 1) % N_GY, coord_z) * BLOCKS + plate_list % BLOCKS
        tower_tiles = jnp.take(block_rows, tower_ids, axis=1)
        plate_tiles = jnp.take(block_rows, plate_ids, axis=1)
        on_tower, on_plate = jax.vmap(pair_terms, in_axes=(1, 1, 0), out_axes=1)(tower_tiles, plate_tiles, mask_list)
        listed = (pair_slots < pair_count).astype(jnp.float32)[None, :, None]
        totals = totals.at[:, tower_ids].add(on_tower * listed)
        totals = totals.at[:, plate_ids].add(on_plate * listed)
        return (totals, None)
    boxes = jnp.arange(DEVICES, dtype=jnp.int32)
    start = jnp.zeros((3, DEVICES * BLOCKS, TILE), jnp.float32)
    totals = lax.scan(one_box, start, (boxes, tower_index, plate_index, tile_counts, exclusions))[0]
    forces_new = totals.reshape(3, DEVICES * BLOCKS * TILE)
    velocity_full = half_kick + 0.5 * time_step * forces_new * inv_mass[None, :]
    departed = jnp.zeros((DEVICES, BLOCKS), jnp.float32).at[boxes[:, None], mig_block].set(1.0)
    staying = jnp.repeat((1.0 - departed).reshape(-1), TILE)[None, :]
    positions_new = moved * staying
    velocities_new = velocity_full * staying
    state = jnp.concatenate([moved, velocity_full], axis=0).reshape(6, DEVICES * BLOCKS, TILE)
    shift_x = jnp.array([-1, -1, -1, 0, 0, 1, 1, 1], dtype=jnp.int32)
    shift_y = jnp.array([-1, 0, 1, -1, 1, -1, 0, 1], dtype=jnp.int32)
    coord_x = boxes // (N_GY * N_GZ)
    coord_y = boxes // N_GZ % N_GY
    coord_z = boxes % N_GZ
    sources = box_number((coord_x[:, None] + shift_x[None, :]) % N_GX, (coord_y[:, None] + shift_y[None, :]) % N_GY, coord_z[:, None])
    source_ids = sources[:, :, None] * BLOCKS + mig_block[sources]
    wanted = (mig_dest[sources] == ((1 - shift_x) * 3 + (1 - shift_y))[None, :, None]).astype(jnp.float32)
    picked = jnp.take(state, source_ids.reshape(-1), axis=1).reshape(6, DEVICES, 8, MIG, TILE)
    arrivals = (picked * wanted[None, :, :, :, None]).reshape(6, DEVICES, 8, MIG * TILE)
    return (positions_new, velocities_new, forces_new, arrivals)
```

```python
import functools

import jax
import jax.numpy as jnp
from jax import lax
from jax.experimental import pallas as pl
from jax.experimental.pallas import tpu as pltpu
from jax.sharding import PartitionSpec as P

time_step = 0.2
soft_core = 0.09
cutoff_sq = 1.44
coulomb_k = 0.5
lanes = 128
sources = ((0, 0), (0, 1), (0, 2), (1, 0), (1, 2), (2, 0), (2, 1), (2, 2))
VMEM_LIMIT = 24 * 1024 * 1024


def neighbours(axis, step):
    count = lax.axis_size(axis)
    return [(i, (i + step) % count) for i in range(count)]


def shift(value, axis, step):
    return lax.ppermute(value, axis, neighbours(axis, step))


def vmem():
    return pl.BlockSpec(memory_space=pltpu.VMEM)


def smem():
    return pl.BlockSpec(memory_space=pltpu.SMEM)


def exact_parts(value):
    high = value.astype(jnp.bfloat16).astype(jnp.float32)
    rest = value - high
    middle = rest.astype(jnp.bfloat16).astype(jnp.float32)
    return high, middle, rest - middle


def pair_kernel(
    length_x,
    length_y,
    unroll,
    tower_list,
    plate_list,
    count,
    towers,
    plates_down,
    plates_own,
    plates_up,
    masks,
    on_towers,
    on_down,
    on_own,
    on_up,
):
    plate_refs = (plates_down, plates_own, plates_up)
    out_refs = (on_down, on_own, on_up)
    blocks = on_towers.shape[1]
    for ref in (on_towers, *out_refs):
        ref[...] = jnp.zeros_like(ref)
    f32 = jnp.float32
    row4 = lax.broadcasted_iota(jnp.int32, (4, lanes), 0)
    lane4 = lax.broadcasted_iota(jnp.int32, (4, lanes), 1)
    sub = lax.broadcasted_iota(jnp.int32, (8, lanes), 0)
    lane = lax.broadcasted_iota(jnp.int32, (8, lanes), 1)
    lane_group = lane // 8
    on_diagonal = sub == lane % 8
    bit = jnp.left_shift(jnp.int32(1), sub)
    scale = jnp.where(
        row4 == 0,
        1.0 / length_x,
        jnp.where(row4 == 1, 1.0 / length_y, jnp.where(row4 == 2, 1.0 / length_x, 1.0)),
    ).astype(f32)
    ratio = (length_y / length_x) ** 2
    unit_sq = length_x * length_x
    soft = soft_core / unit_sq
    fall = unit_sq / cutoff_sq
    tower_scale = jnp.where(row4 == 3, coulomb_k / length_x, scale).astype(f32)
    back = jnp.where(
        row4 == 0,
        length_x / unit_sq,
        jnp.where(row4 == 1, length_y / unit_sq, length_x / unit_sq),
    ).astype(f32)
    pick = jnp.concatenate(
        [
            jnp.where(
                jnp.logical_and(
                    lax.broadcasted_iota(jnp.int32, (16, lanes), 0) % 4 == c,
                    lax.broadcasted_iota(jnp.int32, (16, lanes), 0) < 12,
                ),
                1.0,
                0.0,
            ).astype(f32)
            for c in range(4)
        ],
        axis=1,
    ).astype(jnp.bfloat16)
    total = count[0]

    def one_slot(slot):
        tower, plate = tower_list[0, slot], plate_list[0, slot]
        layer, tower_block = tower // blocks, tower % blocks
        cell, plate_block = plate // blocks, plate % blocks
        cell_x, cell_y = cell // 3, cell % 3
        tower_rows = towers[layer, tower_block] * tower_scale
        tower_kind = towers[layer, blocks]

        def chosen(row):
            found = [ref[cell_x, row] for ref in plate_refs]
            return jnp.where(cell_y == 0, found[0], jnp.where(cell_y == 1, found[1], found[2]))

        plate_rows = chosen(plate_block) * scale
        plate_kind = chosen(blocks)
        of_tower = jnp.sum(
            jnp.where(lane4 == tower_block, tower_kind, 0.0), axis=1, keepdims=True
        )
        of_plate = jnp.sum(
            jnp.where(lane4 == plate_block, plate_kind, 0.0), axis=1, keepdims=True
        )
        sigma = 0.5 * (of_tower[0:1] + of_plate[0:1])
        depth = of_tower[1:2] * of_plate[1:2]
        sigma_sq = sigma * sigma * (1.0 / unit_sq)
        sigma_six = sigma_sq * sigma_sq * sigma_sq
        low = jnp.broadcast_to(6.0 * depth * sigma_six, (8, lanes))
        high = jnp.broadcast_to(12.0 * depth * sigma_six * sigma_six, (8, lanes))
        parts = jnp.concatenate([*exact_parts(plate_rows), jnp.zeros_like(plate_rows)], axis=0)
        spread = lax.dot_general(
            parts.astype(jnp.bfloat16),
            pick,
            (((0,), (0,)), ((), ())),
            preferred_element_type=f32,
        )
        rows = [jnp.broadcast_to(tower_rows[c : c + 1], (8, lanes)) for c in range(4)]
        words = masks[slot]
        on_tower = [jnp.zeros((8, lanes), f32) for _ in range(3)]
        on_plate = [jnp.zeros((8, lanes), f32) for _ in range(3)]
        for w in range(lanes // 8):
            piece = [
                spread[8 * w : 8 * w + 8, lanes * c : lanes * c + lanes] for c in range(4)
            ]
            raw_x, raw_y, dz = (rows[c] - piece[c] for c in range(3))
            dx = raw_x - jnp.round(raw_x)
            dy = raw_y - jnp.round(raw_y)
            dist = dx * dx + ratio * (dy * dy) + dz * dz
            root = lax.rsqrt(dist + soft)
            inverse = root * root
            cube = inverse * inverse * inverse
            falloff = 1.0 - fall * dist
            word = jnp.broadcast_to(words[w : w + 1], (8, lanes))
            falloff = jnp.where(jnp.bitwise_and(word, bit) == 0, falloff, 0.0)
            falloff = jnp.maximum(falloff, 0.0) * root
            energy = cube * (high * cube - low) + rows[3] * piece[3] * root
            strength = energy * (falloff * falloff)
            for c, offset in enumerate((dx, dy, dz)):
                weighted = strength * offset
                on_tower[c] += weighted
                on_plate[c] = jnp.where(
                    lane_group == w, jnp.sum(weighted, axis=1, keepdims=True), on_plate[c]
                )
        listed = jnp.where(slot < total, 1.0, 0.0).astype(f32)
        zero = jnp.zeros((1, lanes), f32)
        tower_sum = jnp.concatenate(
            [*(jnp.sum(v, axis=0, keepdims=True) for v in on_tower), zero], axis=0
        )
        plate_sum = jnp.concatenate(
            [
                *(
                    jnp.sum(jnp.where(on_diagonal, v, 0.0), axis=0, keepdims=True)
                    for v in on_plate
                ),
                zero,
            ],
            axis=0,
        )
        factor = back * listed
        return (
            (layer, tower_block, tower_sum * factor),
            (cell_x, cell_y, plate_block, plate_sum * -factor),
        )

    def step(index, carry):
        done = [one_slot(index * unroll + u) for u in range(unroll)]
        for (layer, tower_block, on_tower), (cell_x, cell_y, plate_block, on_plate) in done:
            on_towers[layer, tower_block] += on_tower
            for y, ref in enumerate(out_refs):
                ref[cell_x, plate_block] += jnp.where(cell_y == y, on_plate, 0.0)
        return carry

    lax.fori_loop(0, (total + unroll - 1) // unroll, step, 0)


def pair_forces(tower_list, plate_list, count, towers, rows, masks, length_x, length_y):
    layers, blocks = towers.shape[0], towers.shape[1] - 1
    shape_row = jax.ShapeDtypeStruct((3, blocks, 4, lanes), jnp.float32)
    return pl.pallas_call(
        functools.partial(pair_kernel, length_x, length_y, 2),
        out_shape=[jax.ShapeDtypeStruct((layers, blocks, 4, lanes), jnp.float32)]
        + [shape_row] * 3,
        in_specs=[smem()] * 3 + [vmem()] * 5,
        out_specs=[vmem()] * 4,
        compiler_params=pltpu.CompilerParams(vmem_limit_bytes=VMEM_LIMIT),
        cost_estimate=pl.CostEstimate(
            flops=40 * 64 * lanes * lanes, bytes_accessed=2**21, transcendentals=64 * lanes * lanes
        ),
        name="pair_forces",
    )(tower_list, plate_list, count, towers, *rows, masks)


def arrival_kernel(down, own, up, out):
    refs = (down, own, up)
    for number, (x, y) in enumerate(sources):
        wanted = float((2 - x) * 3 + (2 - y))
        for q in range(down.shape[1]):
            state = refs[y][x, q]
            kept = jnp.where(state[6:7] == wanted, state, 0.0)
            for c in range(6):
                out[c, number : number + 1, lanes * q : lanes * q + lanes] = kept[c : c + 1]


def arrivals_of(rows):
    leaving = rows[0].shape[1]
    return pl.pallas_call(
        arrival_kernel,
        out_shape=jax.ShapeDtypeStruct((6, 8, leaving * lanes), jnp.float32),
        in_specs=[vmem()] * 3,
        out_specs=vmem(),
        compiler_params=pltpu.CompilerParams(vmem_limit_bytes=VMEM_LIMIT),
        name="arrivals",
    )(*rows)


def by_block(rows):
    return rows.reshape(rows.shape[0], -1, lanes).transpose(1, 0, 2)


def by_atom(tiles):
    return tiles.transpose(1, 0, 2).reshape(tiles.shape[1], -1)


def row_of_three(value):
    return jnp.stack([shift(value, "gx", 1), value, shift(value, "gx", -1)])


def local(
    positions,
    velocities,
    forces_old,
    inv_mass,
    charges,
    block_species,
    sigma_table,
    epsilon_table,
    tower_index,
    plate_index,
    tile_counts,
    exclusions,
    mig_block,
    mig_dest,
):
    atom_count = positions.shape[1]
    block_count = block_species.shape[0]
    layers = lax.axis_size("gz")
    length_x = float(lax.axis_size("gx"))
    length_y = float(lax.axis_size("gy"))
    half_kick = velocities + 0.5 * time_step * forces_old * inv_mass[None, :]
    moved = positions + time_step * half_kick
    kinds = jnp.stack([sigma_table, jnp.sqrt(epsilon_table)])
    per_block = jnp.zeros((2, block_count), jnp.float32)
    for kind in range(sigma_table.shape[0]):
        per_block = jnp.where(block_species[None, :] == kind, kinds[:, kind : kind + 1], per_block)
    kind_tile = jnp.pad(per_block, ((0, 2), (0, lanes - block_count)))
    features = jnp.concatenate(
        [by_block(jnp.concatenate([moved, charges[None, :]])), kind_tile[None]]
    )
    copies = jnp.broadcast_to(features, (layers, *features.shape))
    towers = lax.all_to_all(copies, "gz", split_axis=0, concat_axis=0, tiled=True)
    own = row_of_three(features)
    down, up = shift(own, "gy", 1), shift(own, "gy", -1)
    on_towers, on_down, on_own, on_up = pair_forces(
        tower_index,
        plate_index,
        tile_counts,
        towers,
        (down, own, up),
        exclusions[0],
        length_x,
        length_y,
    )
    tower_back = lax.all_to_all(on_towers, "gz", split_axis=0, concat_axis=0, tiled=True)
    row_sums = on_own + shift(on_down, "gy", -1) + shift(on_up, "gy", 1)
    plate_back = row_sums[1] + shift(row_sums[0], "gx", -1) + shift(row_sums[2], "gx", 1)
    forces_new = by_atom((tower_back.sum(axis=0) + plate_back)[:, 0:3])
    velocity_full = half_kick + 0.5 * time_step * forces_new * inv_mass[None, :]
    leaving = mig_block[0]
    block_slots = jnp.arange(block_count, dtype=jnp.int32)
    departed = jnp.any(leaving[:, None] == block_slots[None, :], axis=0)
    staying = jnp.repeat(1.0 - departed.astype(jnp.float32), lanes)[None, :]
    positions_new = moved * staying
    velocities_new = velocity_full * staying
    tags = jnp.broadcast_to(
        mig_dest[0].astype(jnp.float32)[:, None, None], (leaving.shape[0], 2, lanes)
    )
    state = by_block(jnp.concatenate([moved, velocity_full]))
    state = jnp.concatenate([jnp.take(state, leaving, axis=0), tags], axis=1)
    state_own = row_of_three(state)
    state_down, state_up = shift(state_own, "gy", 1), shift(state_own, "gy", -1)
    arrivals = arrivals_of((state_down, state_own, state_up))[:, None]
    return (positions_new, velocities_new, forces_new, arrivals)


def solution(mesh):
    everywhere = ("gx", "gy", "gz")
    in_specs = (
        P(None, everywhere),
        P(None, everywhere),
        P(None, everywhere),
        P(everywhere),
        P(everywhere),
        P(everywhere),
        P(),
        P(),
        P(everywhere, None),
        P(everywhere, None),
        P(everywhere),
        P(everywhere, None, None, None),
        P(everywhere, None),
        P(everywhere, None),
    )
    out_specs = (
        P(None, everywhere),
        P(None, everywhere),
        P(None, everywhere),
        P(None, everywhere, None, None),
    )
    return jax.shard_map(local, mesh=mesh, in_specs=in_specs, out_specs=out_specs, check_vma=False)
```

```python
import functools

import jax
import jax.numpy as jnp
from jax import lax
from jax.experimental import pallas as pl
from jax.experimental.pallas import tpu as pltpu
from jax.sharding import PartitionSpec as P


time_step = 0.2
soft_core = 0.09
cutoff_sq = 1.44
coulomb_k = 0.5
lanes = 128
sources = ((0, 0), (0, 1), (0, 2), (1, 0), (1, 2), (2, 0), (2, 1), (2, 2))
group = 4
VMEM_LIMIT = 24 * 1024 * 1024


def pairs_first(count):
    return [(i, i + 1) for i in range(0, count, 2)]


def pairs_second(count):
    return [(i, (i + 1) % count) for i in range(1, count, 2)]


def far_pairs(count):
    return [(count // 2 - 1, count // 2), (count - 1, 0)]


def swap(value, axis, pairs):
    return lax.ppermute(value, axis, [*pairs, *((j, i) for i, j in pairs)])


def swap_in_far_rows(value, pairs):
    count = lax.axis_size("gy")
    rows = sorted(y for pair in far_pairs(count) for y in pair)
    return swap(
        value, ("gx", "gy"), [(i * count + y, j * count + y) for i, j in pairs for y in rows]
    )


def halo(value):
    count_x, count_y = lax.axis_size("gx"), lax.axis_size("gy")
    first_x, second_x = pairs_first(count_x), pairs_second(count_x)
    far_y = far_pairs(count_y)
    near_y = [pair for pair in pairs_second(count_y) if pair not in far_y]
    across = swap(value, "gy", far_y)
    own = jnp.stack([swap(value, "gx", first_x), value, swap(value, "gx", second_x)])
    first = swap(own, "gy", pairs_first(count_y))
    second = swap(own, "gy", near_y)
    far = (swap_in_far_rows(across, first_x),
        across,
        swap_in_far_rows(across, second_x),
    )
    return (first, own, second), far


def sent_home(first, own, second):
    count_x, count_y = lax.axis_size("gx"), lax.axis_size("gy")
    first_x, second_x = pairs_first(count_x), pairs_second(count_x)
    far_y = far_pairs(count_y)
    near_y = [pair for pair in pairs_second(count_y) if pair not in far_y]
    side_one = swap_in_far_rows(second[0], first_x)
    side_two = swap_in_far_rows(second[2], second_x)
    across = swap(second[1] + side_one + side_two, "gy", far_y)
    row = own + swap(first, "gy", pairs_first(count_y)) + swap(second, "gy", near_y)
    return row[1] + swap(row[0], "gx", first_x) + swap(row[2], "gx", second_x) + across


def piece_of(offset, odd):
    return jnp.where(offset == 1, 1, jnp.where(offset == 2 * odd, 2, 0))


def vmem():
    return pl.BlockSpec(memory_space=pltpu.VMEM)


def smem():
    return pl.BlockSpec(memory_space=pltpu.SMEM)


def exact_parts(value):
    high = value.astype(jnp.bfloat16).astype(jnp.float32)
    rest = value - high
    middle = rest.astype(jnp.bfloat16).astype(jnp.float32)
    return high, middle, rest - middle


def pair_kernel(
    length_x,
    length_y,
    unroll,
    tower_list,
    plate_list,
    count,
    spot,
    *refs,
):
    tower_refs, (first_row, own_row, second_row), far_refs = refs[0:4], refs[4:7], refs[7:10]
    masks, tower_outs, row_outs, held = refs[10], refs[11:15], refs[15:18], refs[18:]
    blocks = tower_outs[0].shape[0]
    for ref in (*tower_outs, *row_outs):
        ref[...] = jnp.zeros_like(ref)
    odd_x, odd_y, far, me_z = (spot[n] for n in range(4))
    f32 = jnp.float32
    row4 = lax.broadcasted_iota(jnp.int32, (4, lanes), 0)
    lane4 = lax.broadcasted_iota(jnp.int32, (4, lanes), 1)
    sub = lax.broadcasted_iota(jnp.int32, (8, lanes), 0)
    lane = lax.broadcasted_iota(jnp.int32, (8, lanes), 1)
    lane_group = lane // 8
    on_diagonal = sub == lane % 8
    bit = jnp.left_shift(jnp.int32(1), sub)
    scale = jnp.where(
        row4 == 0,
        1.0 / length_x,
        jnp.where(row4 == 1, 1.0 / length_y, jnp.where(row4 == 2, 1.0 / length_x, 1.0)),
    ).astype(f32)
    ratio = (length_y / length_x) ** 2
    unit_sq = length_x * length_x
    soft = soft_core / unit_sq
    fall = unit_sq / cutoff_sq
    tower_scale = jnp.where(row4 == 3, coulomb_k / length_x, scale).astype(f32)
    back = jnp.where(
        row4 == 0,
        length_x / unit_sq,
        jnp.where(row4 == 1, length_y / unit_sq, length_x / unit_sq),
    ).astype(f32)
    pick = jnp.concatenate(
        [
            jnp.where(
                jnp.logical_and(
                    lax.broadcasted_iota(jnp.int32, (16, lanes), 0) % 4 == c,
                    lax.broadcasted_iota(jnp.int32, (16, lanes), 0) < 12,
                ),
                1.0,
                0.0,
            ).astype(f32)
            for c in range(4)
        ],
        axis=1,
    ).astype(jnp.bfloat16)
    total = count[0]

    def place(slot):
        tower, plate = tower_list[0, slot], plate_list[0, slot]
        cell = plate // blocks
        return (
            jnp.bitwise_xor(tower // blocks, me_z),
            tower % blocks,
            piece_of(cell // 3, odd_x),
            piece_of(cell % 3, odd_y),
            plate % blocks,
        )

    def tower_tile(layer, row):
        near = jnp.where(layer == 0, tower_refs[0][row], tower_refs[1][row])
        return jnp.where(
            layer < 2, near, jnp.where(layer == 2, tower_refs[2][row], tower_refs[3][row])
        )

    last = tower_list.shape[1] - 1

    def prepare(slot, buffer, u):
        spread_ref, terms_ref = buffer
        layer, tower_block, cell_x, cell_y, plate_block = place(jnp.minimum(slot, last))
        tower_kind = tower_tile(layer, blocks)

        def chosen(row):
            from_far = jnp.where(
                cell_x == 0,
                far_refs[0][row],
                jnp.where(cell_x == 1, far_refs[1][row], far_refs[2][row]),
            )
            second = jnp.where(far == 1, from_far, second_row[cell_x, row])
            return jnp.where(
                cell_y == 0,
                first_row[cell_x, row],
                jnp.where(cell_y == 1, own_row[cell_x, row], second),
            )

        plate_rows = chosen(plate_block) * scale
        plate_kind = chosen(blocks)
        of_tower = jnp.sum(
            jnp.where(lane4 == tower_block, tower_kind, 0.0), axis=1, keepdims=True
        )
        of_plate = jnp.sum(
            jnp.where(lane4 == plate_block, plate_kind, 0.0), axis=1, keepdims=True
        )
        sigma = 0.5 * (of_tower[0:1] + of_plate[0:1])
        depth = of_tower[1:2] * of_plate[1:2]
        sigma_sq = sigma * sigma * (1.0 / unit_sq)
        sigma_six = sigma_sq * sigma_sq * sigma_sq
        low = jnp.broadcast_to(6.0 * depth * sigma_six, (8, lanes))
        high = jnp.broadcast_to(12.0 * depth * sigma_six * sigma_six, (8, lanes))
        parts = jnp.concatenate([*exact_parts(plate_rows), jnp.zeros_like(plate_rows)], axis=0)
        spread_ref[u] = lax.dot_general(
            parts.astype(jnp.bfloat16),
            pick,
            (((0,), (0,)), ((), ())),
            preferred_element_type=f32,
        )
        terms_ref[u, 0] = low
        terms_ref[u, 1] = high

    def evaluate(slot, buffer, u):
        spread_ref, terms_ref = buffer
        layer, tower_block, cell_x, cell_y, plate_block = place(slot)
        tower_rows = tower_tile(layer, tower_block) * tower_scale
        low, high = terms_ref[u, 0], terms_ref[u, 1]
        rows = [jnp.broadcast_to(tower_rows[c : c + 1], (8, lanes)) for c in range(4)]
        words = masks[slot]
        on_tower = [jnp.zeros((8, lanes), f32) for _ in range(3)]
        on_plate = [jnp.zeros((8, lanes), f32) for _ in range(3)]
        for w in range(lanes // 8):
            piece = [
                spread_ref[u, 8 * w : 8 * w + 8, lanes * c : lanes * c + lanes]
                for c in range(4)
            ]
            raw_x, raw_y, dz = (rows[c] - piece[c] for c in range(3))
            dx = raw_x - jnp.round(raw_x)
            dy = raw_y - jnp.round(raw_y)
            dist = dx * dx + ratio * (dy * dy) + dz * dz
            root = lax.rsqrt(dist + soft)
            inverse = root * root
            cube = inverse * inverse * inverse
            falloff = 1.0 - fall * dist
            word = jnp.broadcast_to(words[w : w + 1], (8, lanes))
            falloff = jnp.where(jnp.bitwise_and(word, bit) == 0, falloff, 0.0)
            falloff = jnp.maximum(falloff, 0.0) * root
            energy = cube * (high * cube - low) + rows[3] * piece[3] * root
            strength = energy * (falloff * falloff)
            for c, offset in enumerate((dx, dy, dz)):
                weighted = strength * offset
                on_tower[c] += weighted
                on_plate[c] = jnp.where(
                    lane_group == w, jnp.sum(weighted, axis=1, keepdims=True), on_plate[c]
                )
        listed = jnp.where(slot < total, 1.0, 0.0).astype(f32)
        zero = jnp.zeros((1, lanes), f32)
        tower_sum = jnp.concatenate(
            [*(jnp.sum(v, axis=0, keepdims=True) for v in on_tower), zero], axis=0
        )
        plate_sum = jnp.concatenate(
            [
                *(
                    jnp.sum(jnp.where(on_diagonal, v, 0.0), axis=0, keepdims=True)
                    for v in on_plate
                ),
                zero,
            ],
            axis=0,
        )
        factor = back * listed
        return (
            (layer, tower_block, tower_sum * factor),
            (cell_x, cell_y, plate_block, plate_sum * -factor),
        )

    def finish(done):
        for (layer, tower_block, on_tower), (cell_x, cell_y, plate_block, on_plate) in done:
            for z, ref in enumerate(tower_outs):
                ref[tower_block] += jnp.where(layer == z, on_tower, 0.0)
            for y, ref in enumerate(row_outs):
                ref[cell_x, plate_block] += jnp.where(cell_y == y, on_plate, 0.0)

    buffers = (held[0:2], held[2:4])

    def step(index, carry):
        done = []
        for half in range(2):
            first = (2 * index + half) * unroll
            for u in range(unroll):
                prepare(first + unroll + u, buffers[1 - half], u)
            done += [evaluate(first + u, buffers[half], u) for u in range(unroll)]
        finish(done)
        return carry

    for u in range(unroll):
        prepare(u, buffers[0], u)
    lax.fori_loop(0, (total + 2 * unroll - 1) // (2 * unroll), step, 0)


def pair_forces(tower_list, plate_list, count, spot, towers, rows, far, masks, lengths):
    blocks = towers[0].shape[0] - 1
    shape_one = jax.ShapeDtypeStruct((blocks, 4, lanes), jnp.float32)
    shape_row = jax.ShapeDtypeStruct((3, blocks, 4, lanes), jnp.float32)
    return pl.pallas_call(
        functools.partial(pair_kernel, *lengths, group),
        out_shape=[shape_one] * 4 + [shape_row] * 3,
        in_specs=[smem()] * 4 + [vmem()] * 11,
        out_specs=[vmem()] * 7,
        scratch_shapes=[
            pltpu.VMEM((group, lanes, 4 * lanes), jnp.float32),
            pltpu.VMEM((group, 2, 8, lanes), jnp.float32),
        ]
        * 2,
        compiler_params=pltpu.CompilerParams(vmem_limit_bytes=VMEM_LIMIT),
        cost_estimate=pl.CostEstimate(
            flops=40 * 64 * lanes * lanes, bytes_accessed=2**21, transcendentals=64 * lanes * lanes
        ),
        name="pair_forces",
    )(tower_list, plate_list, count, spot, *towers, *rows, *far, masks)


def arrival_kernel(spot, *refs):
    (first_row, own_row, second_row), far_refs, out = refs[0:3], refs[3:6], refs[6]
    odd_x, odd_y, far = spot[0], spot[1], spot[2]
    for q in range(own_row.shape[1]):
        second = [jnp.where(far == 1, far_refs[k][q], second_row[k, q]) for k in range(3)]
        first = [first_row[k, q] for k in range(3)]
        own = [own_row[k, q] for k in range(3)]
        for number, (x, y) in enumerate(sources):
            wanted = float((2 - x) * 3 + (2 - y))
            by_y = own
            if y != 1:
                flip = odd_y == (1 if y == 0 else 0)
                by_y = [jnp.where(flip, first[k], second[k]) for k in range(3)]
            state = by_y[1]
            if x != 1:
                flip = odd_x == (1 if x == 0 else 0)
                state = jnp.where(flip, by_y[0], by_y[2])
            kept = jnp.where(state[6:7] == wanted, state, 0.0)
            for c in range(6):
                out[c, number : number + 1, lanes * q : lanes * q + lanes] = kept[c : c + 1]


def arrivals_of(spot, rows, far):
    leaving = rows[0].shape[1]
    return pl.pallas_call(
        arrival_kernel,
        out_shape=jax.ShapeDtypeStruct((6, 8, leaving * lanes), jnp.float32),
        in_specs=[smem()] + [vmem()] * 6,
        out_specs=vmem(),
        compiler_params=pltpu.CompilerParams(vmem_limit_bytes=VMEM_LIMIT),
        name="arrivals",
    )(spot, *rows, *far)


def by_block(rows):
    return rows.reshape(rows.shape[0], -1, lanes).transpose(1, 0, 2)


def by_atom(tiles):
    return tiles.transpose(1, 0, 2).reshape(tiles.shape[1], -1)


def local(
    positions,
    velocities,
    forces_old,
    inv_mass,
    charges,
    block_species,
    sigma_table,
    epsilon_table,
    tower_index,
    plate_index,
    tile_counts,
    exclusions,
    mig_block,
    mig_dest,
):
    block_count = block_species.shape[0]
    layers = lax.axis_size("gz")
    length_x = float(lax.axis_size("gx"))
    length_y = float(lax.axis_size("gy"))
    half_kick = velocities + 0.5 * time_step * forces_old * inv_mass[None, :]
    moved = positions + time_step * half_kick
    kinds = jnp.stack([sigma_table, jnp.sqrt(epsilon_table)])
    per_block = jnp.zeros((2, block_count), jnp.float32)
    for kind in range(sigma_table.shape[0]):
        per_block = jnp.where(block_species[None, :] == kind, kinds[:, kind : kind + 1], per_block)
    kind_tile = jnp.pad(per_block, ((0, 2), (0, lanes - block_count)))
    features = jnp.concatenate(
        [by_block(jnp.concatenate([moved, charges[None, :]])), kind_tile[None]]
    )
    count_y = lax.axis_size("gy")
    me_x, me_y, me_z = (lax.axis_index(axis) for axis in ("gx", "gy", "gz"))
    is_far = functools.reduce(
        jnp.logical_or, [me_y == y for pair in far_pairs(count_y) for y in pair]
    )
    spot = jnp.stack([me_x % 2, me_y % 2, is_far.astype(jnp.int32), me_z]).astype(jnp.int32)
    rows, far = halo(features)

    def from_layer(value, step):
        return lax.ppermute(value, "gz", [(i, i ^ step) for i in range(layers)])

    towers = [features] + [from_layer(features, step) for step in range(1, layers)]
    sums = pair_forces(
        tower_index,
        plate_index,
        tile_counts,
        spot,
        towers,
        rows,
        far,
        exclusions[0],
        (length_x, length_y),
    )
    tower_back = sums[0] + sum(from_layer(sums[step], step) for step in range(1, layers))
    total = tower_back + sent_home(*sums[layers:])
    forces_new = by_atom(total[:, 0:3])
    velocity_full = half_kick + 0.5 * time_step * forces_new * inv_mass[None, :]
    leaving = mig_block[0]
    block_slots = jnp.arange(block_count, dtype=jnp.int32)
    departed = jnp.any(leaving[:, None] == block_slots[None, :], axis=0)
    staying = jnp.repeat(1.0 - departed.astype(jnp.float32), lanes)[None, :]
    positions_new = moved * staying
    velocities_new = velocity_full * staying
    tags = jnp.broadcast_to(
        mig_dest[0].astype(jnp.float32)[:, None, None], (leaving.shape[0], 2, lanes)
    )
    state = by_block(jnp.concatenate([moved, velocity_full]))
    state = jnp.concatenate([jnp.take(state, leaving, axis=0), tags], axis=1)
    arrivals = arrivals_of(spot, *halo(state))[:, None]
    return (positions_new, velocities_new, forces_new, arrivals)


def solution(mesh):
    everywhere = ("gx", "gy", "gz")
    in_specs = (
        P(None, everywhere),
        P(None, everywhere),
        P(None, everywhere),
        P(everywhere),
        P(everywhere),
        P(everywhere),
        P(),
        P(),
        P(everywhere, None),
        P(everywhere, None),
        P(everywhere),
        P(everywhere, None, None, None),
        P(everywhere, None),
        P(everywhere, None),
    )
    out_specs = (
        P(None, everywhere),
        P(None, everywhere),
        P(None, everywhere),
        P(None, everywhere, None, None),
    )
    return jax.shard_map(local, mesh=mesh, in_specs=in_specs, out_specs=out_specs, check_vma=False)
```

```python
import functools

import jax
import jax.numpy as jnp
from jax import lax
from jax.experimental import pallas as pl
from jax.experimental.pallas import tpu as pltpu
from jax.sharding import PartitionSpec as P


time_step = 0.2
soft_core = 0.09
cutoff_sq = 1.44
coulomb_k = 0.5
lanes = 128
sources = ((0, 0), (0, 1), (0, 2), (1, 0), (1, 2), (2, 0), (2, 1), (2, 2))
group = 4
VMEM_LIMIT = 24 * 1024 * 1024


def pairs_first(count):
    return [(i, i + 1) for i in range(0, count, 2)]


def pairs_second(count):
    return [(i, (i + 1) % count) for i in range(1, count, 2)]


def swap(value, axis, pairs):
    return lax.ppermute(value, axis, [*pairs, *((j, i) for i, j in pairs)])


def halo(value):
    count_x, count_y = lax.axis_size("gx"), lax.axis_size("gy")
    own = jnp.stack(
        [swap(value, "gx", pairs_first(count_x)), value, swap(value, "gx", pairs_second(count_x))]
    )
    return (swap(own, "gy", pairs_first(count_y)), own, swap(own, "gy", pairs_second(count_y)))


def sent_home(first, own, second):
    count_x, count_y = lax.axis_size("gx"), lax.axis_size("gy")
    row = (
        own
        + swap(first, "gy", pairs_first(count_y))
        + swap(second, "gy", pairs_second(count_y))
    )
    return (
        row[1]
        + swap(row[0], "gx", pairs_first(count_x))
        + swap(row[2], "gx", pairs_second(count_x))
    )


def piece_of(offset, odd):
    return jnp.where(offset == 1, 1, jnp.where(offset == 2 * odd, 2, 0))


def vmem():
    return pl.BlockSpec(memory_space=pltpu.VMEM)


def smem():
    return pl.BlockSpec(memory_space=pltpu.SMEM)


def exact_parts(value):
    high = value.astype(jnp.bfloat16).astype(jnp.float32)
    rest = value - high
    middle = rest.astype(jnp.bfloat16).astype(jnp.float32)
    return high, middle, rest - middle


def pair_kernel(
    length_x,
    length_y,
    unroll,
    tower_list,
    plate_list,
    count,
    spot,
    *refs,
):
    tower_refs, (first_row, own_row, second_row) = refs[0:4], refs[4:7]
    masks, tower_outs, row_outs, held = refs[7], refs[8:12], refs[12:15], refs[15:]
    blocks = tower_outs[0].shape[0]
    for ref in (*tower_outs, *row_outs):
        ref[...] = jnp.zeros_like(ref)
    odd_x, odd_y, me_z = (spot[n] for n in range(3))
    f32 = jnp.float32
    row4 = lax.broadcasted_iota(jnp.int32, (4, lanes), 0)
    lane4 = lax.broadcasted_iota(jnp.int32, (4, lanes), 1)
    sub = lax.broadcasted_iota(jnp.int32, (8, lanes), 0)
    lane = lax.broadcasted_iota(jnp.int32, (8, lanes), 1)
    lane_group = lane // 8
    on_diagonal = sub == lane % 8
    bit = jnp.left_shift(jnp.int32(1), sub)
    scale = jnp.where(
        row4 == 0,
        1.0 / length_x,
        jnp.where(row4 == 1, 1.0 / length_y, jnp.where(row4 == 2, 1.0 / length_x, 1.0)),
    ).astype(f32)
    ratio = (length_y / length_x) ** 2
    unit_sq = length_x * length_x
    soft = soft_core / unit_sq
    fall = unit_sq / cutoff_sq
    tower_scale = jnp.where(row4 == 3, coulomb_k / length_x, scale).astype(f32)
    back = jnp.where(
        row4 == 0,
        length_x / unit_sq,
        jnp.where(row4 == 1, length_y / unit_sq, length_x / unit_sq),
    ).astype(f32)
    pick = jnp.concatenate(
        [
            jnp.where(
                jnp.logical_and(
                    lax.broadcasted_iota(jnp.int32, (16, lanes), 0) % 4 == c,
                    lax.broadcasted_iota(jnp.int32, (16, lanes), 0) < 12,
                ),
                1.0,
                0.0,
            ).astype(f32)
            for c in range(4)
        ],
        axis=1,
    ).astype(jnp.bfloat16)
    total = count[0]

    def place(slot):
        tower, plate = tower_list[0, slot], plate_list[0, slot]
        cell = plate // blocks
        return (
            jnp.bitwise_xor(tower // blocks, me_z),
            tower % blocks,
            piece_of(cell // 3, odd_x),
            piece_of(cell % 3, odd_y),
            plate % blocks,
        )

    def tower_tile(layer, row):
        near = jnp.where(layer == 0, tower_refs[0][row], tower_refs[1][row])
        return jnp.where(
            layer < 2, near, jnp.where(layer == 2, tower_refs[2][row], tower_refs[3][row])
        )

    last = tower_list.shape[1] - 1

    def prepare(slot, buffer, u):
        spread_ref, terms_ref = buffer
        layer, tower_block, cell_x, cell_y, plate_block = place(jnp.minimum(slot, last))
        tower_kind = tower_tile(layer, blocks)

        def chosen(row):
            return jnp.where(
                cell_y == 0,
                first_row[cell_x, row],
                jnp.where(cell_y == 1, own_row[cell_x, row], second_row[cell_x, row]),
            )

        plate_rows = chosen(plate_block) * scale
        plate_kind = chosen(blocks)
        of_tower = jnp.sum(
            jnp.where(lane4 == tower_block, tower_kind, 0.0), axis=1, keepdims=True
        )
        of_plate = jnp.sum(
            jnp.where(lane4 == plate_block, plate_kind, 0.0), axis=1, keepdims=True
        )
        sigma = 0.5 * (of_tower[0:1] + of_plate[0:1])
        depth = of_tower[1:2] * of_plate[1:2]
        sigma_sq = sigma * sigma * (1.0 / unit_sq)
        sigma_six = sigma_sq * sigma_sq * sigma_sq
        low = jnp.broadcast_to(6.0 * depth * sigma_six, (8, lanes))
        high = jnp.broadcast_to(12.0 * depth * sigma_six * sigma_six, (8, lanes))
        parts = jnp.concatenate([*exact_parts(plate_rows), jnp.zeros_like(plate_rows)], axis=0)
        spread_ref[u] = lax.dot_general(
            parts.astype(jnp.bfloat16),
            pick,
            (((0,), (0,)), ((), ())),
            preferred_element_type=f32,
        )
        terms_ref[u, 0] = low
        terms_ref[u, 1] = high

    def evaluate(slot, buffer, u):
        spread_ref, terms_ref = buffer
        layer, tower_block, cell_x, cell_y, plate_block = place(slot)
        tower_rows = tower_tile(layer, tower_block) * tower_scale
        low, high = terms_ref[u, 0], terms_ref[u, 1]
        rows = [jnp.broadcast_to(tower_rows[c : c + 1], (8, lanes)) for c in range(4)]
        words = masks[slot]
        on_tower = [jnp.zeros((8, lanes), f32) for _ in range(3)]
        on_plate = [jnp.zeros((8, lanes), f32) for _ in range(3)]
        for w in range(lanes // 8):
            piece = [
                spread_ref[u, 8 * w : 8 * w + 8, lanes * c : lanes * c + lanes]
                for c in range(4)
            ]
            raw_x, raw_y, dz = (rows[c] - piece[c] for c in range(3))
            dx = raw_x - jnp.round(raw_x)
            dy = raw_y - jnp.round(raw_y)
            dist = dx * dx + ratio * (dy * dy) + dz * dz
            root = lax.rsqrt(dist + soft)
            inverse = root * root
            cube = inverse * inverse * inverse
            falloff = 1.0 - fall * dist
            word = jnp.broadcast_to(words[w : w + 1], (8, lanes))
            falloff = jnp.where(jnp.bitwise_and(word, bit) == 0, falloff, 0.0)
            falloff = jnp.maximum(falloff, 0.0) * root
            energy = cube * (high * cube - low) + rows[3] * piece[3] * root
            strength = energy * (falloff * falloff)
            for c, offset in enumerate((dx, dy, dz)):
                weighted = strength * offset
                on_tower[c] += weighted
                on_plate[c] = jnp.where(
                    lane_group == w, jnp.sum(weighted, axis=1, keepdims=True), on_plate[c]
                )
        listed = jnp.where(slot < total, 1.0, 0.0).astype(f32)
        zero = jnp.zeros((1, lanes), f32)
        tower_sum = jnp.concatenate(
            [*(jnp.sum(v, axis=0, keepdims=True) for v in on_tower), zero], axis=0
        )
        plate_sum = jnp.concatenate(
            [
                *(
                    jnp.sum(jnp.where(on_diagonal, v, 0.0), axis=0, keepdims=True)
                    for v in on_plate
                ),
                zero,
            ],
            axis=0,
        )
        factor = back * listed
        return (
            (layer, tower_block, tower_sum * factor),
            (cell_x, cell_y, plate_block, plate_sum * -factor),
        )

    def finish(done):
        for (layer, tower_block, on_tower), (cell_x, cell_y, plate_block, on_plate) in done:
            for z, ref in enumerate(tower_outs):
                ref[tower_block] += jnp.where(layer == z, on_tower, 0.0)
            for y, ref in enumerate(row_outs):
                ref[cell_x, plate_block] += jnp.where(cell_y == y, on_plate, 0.0)

    buffers = (held[0:2], held[2:4])

    def step(index, carry):
        done = []
        for half in range(2):
            first = (2 * index + half) * unroll
            for u in range(unroll):
                prepare(first + unroll + u, buffers[1 - half], u)
            done += [evaluate(first + u, buffers[half], u) for u in range(unroll)]
        finish(done)
        return carry

    for u in range(unroll):
        prepare(u, buffers[0], u)
    lax.fori_loop(0, (total + 2 * unroll - 1) // (2 * unroll), step, 0)


def pair_forces(tower_list, plate_list, count, spot, towers, rows, masks, lengths):
    blocks = towers[0].shape[0] - 1
    shape_one = jax.ShapeDtypeStruct((blocks, 4, lanes), jnp.float32)
    shape_row = jax.ShapeDtypeStruct((3, blocks, 4, lanes), jnp.float32)
    return pl.pallas_call(
        functools.partial(pair_kernel, *lengths, group),
        out_shape=[shape_one] * 4 + [shape_row] * 3,
        in_specs=[smem()] * 4 + [vmem()] * 8,
        out_specs=[vmem()] * 7,
        scratch_shapes=[
            pltpu.VMEM((group, lanes, 4 * lanes), jnp.float32),
            pltpu.VMEM((group, 2, 8, lanes), jnp.float32),
        ]
        * 2,
        compiler_params=pltpu.CompilerParams(vmem_limit_bytes=VMEM_LIMIT),
        cost_estimate=pl.CostEstimate(
            flops=40 * 64 * lanes * lanes, bytes_accessed=2**21, transcendentals=64 * lanes * lanes
        ),
        name="pair_forces",
    )(tower_list, plate_list, count, spot, *towers, *rows, masks)


def arrival_kernel(spot, *refs):
    first_row, own_row, second_row, out = refs
    odd_x, odd_y = spot[0], spot[1]
    for q in range(own_row.shape[1]):
        second = [second_row[k, q] for k in range(3)]
        first = [first_row[k, q] for k in range(3)]
        own = [own_row[k, q] for k in range(3)]
        for number, (x, y) in enumerate(sources):
            wanted = float((2 - x) * 3 + (2 - y))
            by_y = own
            if y != 1:
                flip = odd_y == (1 if y == 0 else 0)
                by_y = [jnp.where(flip, first[k], second[k]) for k in range(3)]
            state = by_y[1]
            if x != 1:
                flip = odd_x == (1 if x == 0 else 0)
                state = jnp.where(flip, by_y[0], by_y[2])
            kept = jnp.where(state[6:7] == wanted, state, 0.0)
            for c in range(6):
                out[c, number : number + 1, lanes * q : lanes * q + lanes] = kept[c : c + 1]


def arrivals_of(spot, rows):
    leaving = rows[0].shape[1]
    return pl.pallas_call(
        arrival_kernel,
        out_shape=jax.ShapeDtypeStruct((6, 8, leaving * lanes), jnp.float32),
        in_specs=[smem()] + [vmem()] * 3,
        out_specs=vmem(),
        compiler_params=pltpu.CompilerParams(vmem_limit_bytes=VMEM_LIMIT),
        name="arrivals",
    )(spot, *rows)


def by_block(rows):
    return rows.reshape(rows.shape[0], -1, lanes).transpose(1, 0, 2)


def by_atom(tiles):
    return tiles.transpose(1, 0, 2).reshape(tiles.shape[1], -1)


def local(
    positions,
    velocities,
    forces_old,
    inv_mass,
    charges,
    block_species,
    sigma_table,
    epsilon_table,
    tower_index,
    plate_index,
    tile_counts,
    exclusions,
    mig_block,
    mig_dest,
):
    block_count = block_species.shape[0]
    layers = lax.axis_size("gz")
    length_x = float(lax.axis_size("gx"))
    length_y = float(lax.axis_size("gy"))
    half_kick = velocities + 0.5 * time_step * forces_old * inv_mass[None, :]
    moved = positions + time_step * half_kick
    kinds = jnp.stack([sigma_table, jnp.sqrt(epsilon_table)])
    per_block = jnp.zeros((2, block_count), jnp.float32)
    for kind in range(sigma_table.shape[0]):
        per_block = jnp.where(block_species[None, :] == kind, kinds[:, kind : kind + 1], per_block)
    kind_tile = jnp.pad(per_block, ((0, 2), (0, lanes - block_count)))
    features = jnp.concatenate(
        [by_block(jnp.concatenate([moved, charges[None, :]])), kind_tile[None]]
    )
    me_x, me_y, me_z = (lax.axis_index(axis) for axis in ("gx", "gy", "gz"))
    spot = jnp.stack([me_x % 2, me_y % 2, me_z]).astype(jnp.int32)
    rows = halo(features)

    def from_layer(value, step):
        return lax.ppermute(value, "gz", [(i, i ^ step) for i in range(layers)])

    towers = [features] + [from_layer(features, step) for step in range(1, layers)]
    sums = pair_forces(
        tower_index,
        plate_index,
        tile_counts,
        spot,
        towers,
        rows,
        exclusions[0],
        (length_x, length_y),
    )
    tower_back = sums[0] + sum(from_layer(sums[step], step) for step in range(1, layers))
    total = tower_back + sent_home(*sums[layers:])
    forces_new = by_atom(total[:, 0:3])
    velocity_full = half_kick + 0.5 * time_step * forces_new * inv_mass[None, :]
    leaving = mig_block[0]
    block_slots = jnp.arange(block_count, dtype=jnp.int32)
    departed = jnp.any(leaving[:, None] == block_slots[None, :], axis=0)
    staying = jnp.repeat(1.0 - departed.astype(jnp.float32), lanes)[None, :]
    positions_new = moved * staying
    velocities_new = velocity_full * staying
    tags = jnp.broadcast_to(
        mig_dest[0].astype(jnp.float32)[:, None, None], (leaving.shape[0], 2, lanes)
    )
    state = by_block(jnp.concatenate([moved, velocity_full]))
    state = jnp.concatenate([jnp.take(state, leaving, axis=0), tags], axis=1)
    arrivals = arrivals_of(spot, halo(state))[:, None]
    return (positions_new, velocities_new, forces_new, arrivals)


def solution(mesh):
    everywhere = ("gx", "gy", "gz")
    in_specs = (
        P(None, everywhere),
        P(None, everywhere),
        P(None, everywhere),
        P(everywhere),
        P(everywhere),
        P(everywhere),
        P(),
        P(),
        P(everywhere, None),
        P(everywhere, None),
        P(everywhere),
        P(everywhere, None, None, None),
        P(everywhere, None),
        P(everywhere, None),
    )
    out_specs = (
        P(None, everywhere),
        P(None, everywhere),
        P(None, everywhere),
        P(None, everywhere, None, None),
    )
    return jax.shard_map(local, mesh=mesh, in_specs=in_specs, out_specs=out_specs, check_vma=False)
```

```python
import functools

import jax
import jax.numpy as jnp
from jax import lax
from jax.experimental import pallas as pl
from jax.experimental.pallas import tpu as pltpu
from jax.sharding import PartitionSpec as P


time_step = 0.2
soft_core = 0.09
cutoff_sq = 1.44
coulomb_k = 0.5
lanes = 128
sources = ((0, 0), (0, 1), (0, 2), (1, 0), (1, 2), (2, 0), (2, 1), (2, 2))
group = 4
VMEM_LIMIT = 24 * 1024 * 1024


def pairs_first(count):
    return [(i, i + 1) for i in range(0, count, 2)]


def pairs_second(count):
    return [(i, (i + 1) % count) for i in range(1, count, 2)]


def swap(value, axis, pairs):
    return lax.ppermute(value, axis, [*pairs, *((j, i) for i, j in pairs)])


def halo(value):
    count_x, count_y = lax.axis_size("gx"), lax.axis_size("gy")
    own = jnp.stack(
        [swap(value, "gx", pairs_first(count_x)), value, swap(value, "gx", pairs_second(count_x))]
    )
    return (swap(own, "gy", pairs_first(count_y)), own, swap(own, "gy", pairs_second(count_y)))


def sent_home(first, own, second):
    count_x, count_y = lax.axis_size("gx"), lax.axis_size("gy")
    row = (
        own
        + swap(first, "gy", pairs_first(count_y))
        + swap(second, "gy", pairs_second(count_y))
    )
    return [
        row[1], swap(row[0], "gx", pairs_first(count_x)), swap(row[2], "gx", pairs_second(count_x))
    ]


def piece_of(offset, odd):
    return jnp.where(offset == 1, 1, jnp.where(offset == 2 * odd, 2, 0))


def vmem():
    return pl.BlockSpec(memory_space=pltpu.VMEM)


def smem():
    return pl.BlockSpec(memory_space=pltpu.SMEM)


def exact_parts(value):
    high = value.astype(jnp.bfloat16).astype(jnp.float32)
    rest = value - high
    middle = rest.astype(jnp.bfloat16).astype(jnp.float32)
    return high, middle, rest - middle


def pair_kernel(
    length_x,
    length_y,
    unroll,
    tower_list,
    plate_list,
    count,
    spot,
    sigma_table,
    epsilon_table,
    *refs,
):
    tower_refs, (first_row, own_row, second_row) = refs[0:4], refs[4:7]
    masks, tower_outs, row_outs, held = refs[7], refs[8:12], refs[12:15], refs[15:]
    blocks = tower_outs[0].shape[0]
    for ref in (*tower_outs, *row_outs):
        ref[...] = jnp.zeros_like(ref)
    odd_x, odd_y, me_z = (spot[n] for n in range(3))
    f32 = jnp.float32
    row4 = lax.broadcasted_iota(jnp.int32, (4, lanes), 0)
    lane4 = lax.broadcasted_iota(jnp.int32, (4, lanes), 1)
    sub = lax.broadcasted_iota(jnp.int32, (8, lanes), 0)
    lane = lax.broadcasted_iota(jnp.int32, (8, lanes), 1)
    lane_group = lane // 8
    on_diagonal = sub == lane % 8
    bit = jnp.left_shift(jnp.int32(1), sub)
    scale = jnp.where(
        row4 == 0,
        1.0 / length_x,
        jnp.where(row4 == 1, 1.0 / length_y, jnp.where(row4 == 2, 1.0 / length_x, 1.0)),
    ).astype(f32)
    ratio = (length_y / length_x) ** 2
    unit_sq = length_x * length_x
    soft = soft_core / unit_sq
    fall = unit_sq / cutoff_sq
    tower_scale = jnp.where(row4 == 3, coulomb_k / length_x, scale).astype(f32)
    back = jnp.where(
        row4 == 0,
        length_x / unit_sq,
        jnp.where(row4 == 1, length_y / unit_sq, length_x / unit_sq),
    ).astype(f32)
    pick = jnp.concatenate(
        [
            jnp.where(
                jnp.logical_and(
                    lax.broadcasted_iota(jnp.int32, (16, lanes), 0) % 4 == c,
                    lax.broadcasted_iota(jnp.int32, (16, lanes), 0) < 12,
                ),
                1.0,
                0.0,
            ).astype(f32)
            for c in range(4)
        ],
        axis=1,
    ).astype(jnp.bfloat16)
    total = count[0]
    sigmas = [jnp.full((1, 1), sigma_table[n]) for n in range(sigma_table.shape[0])]
    depths = [jnp.sqrt(jnp.full((1, 1), epsilon_table[n])) for n in range(sigma_table.shape[0])]

    def of_kind(table, kind):
        value = table[0]
        for n in range(1, len(table)):
            value = jnp.where(kind == n, table[n], value)
        return value


    shift = blocks.bit_length() - 1

    def place(slot):
        tower, plate = tower_list[0, slot], plate_list[0, slot]
        cell = jnp.right_shift(plate, shift)
        cell_x = jnp.right_shift(cell * 11, 5)
        return (
            jnp.bitwise_xor(jnp.right_shift(tower, shift), me_z),
            jnp.bitwise_and(tower, blocks - 1),
            piece_of(cell_x, odd_x),
            piece_of(cell - 3 * cell_x, odd_y),
            jnp.bitwise_and(plate, blocks - 1),
        )

    def tower_tile(layer, row):
        near = jnp.where(layer == 0, tower_refs[0][row], tower_refs[1][row])
        return jnp.where(
            layer < 2, near, jnp.where(layer == 2, tower_refs[2][row], tower_refs[3][row])
        )

    last = tower_list.shape[1] - 1

    def prepare(slot, buffer, u):
        spread_ref, terms_ref = buffer
        layer, tower_block, cell_x, cell_y, plate_block = place(jnp.minimum(slot, last))
        tower_kind = tower_tile(layer, blocks)

        def chosen(row):
            return jnp.where(
                cell_y == 0,
                first_row[cell_x, row],
                jnp.where(cell_y == 1, own_row[cell_x, row], second_row[cell_x, row]),
            )

        plate_rows = chosen(plate_block) * scale
        plate_kind = chosen(blocks)
        of_tower = jnp.sum(
            jnp.where(lane4 == tower_block, tower_kind, 0.0), axis=1, keepdims=True
        )
        of_plate = jnp.sum(
            jnp.where(lane4 == plate_block, plate_kind, 0.0), axis=1, keepdims=True
        )
        kind_one, kind_two = of_tower[0:1], of_plate[0:1]
        sigma = 0.5 * (of_kind(sigmas, kind_one) + of_kind(sigmas, kind_two))
        depth = of_kind(depths, kind_one) * of_kind(depths, kind_two)
        sigma_sq = sigma * sigma * (1.0 / unit_sq)
        sigma_six = sigma_sq * sigma_sq * sigma_sq
        low = jnp.broadcast_to(6.0 * depth * sigma_six, (8, lanes))
        high = jnp.broadcast_to(12.0 * depth * sigma_six * sigma_six, (8, lanes))
        parts = jnp.concatenate([*exact_parts(plate_rows), jnp.zeros_like(plate_rows)], axis=0)
        spread_ref[u] = lax.dot_general(
            parts.astype(jnp.bfloat16),
            pick,
            (((0,), (0,)), ((), ())),
            preferred_element_type=f32,
        )
        terms_ref[u, 0] = low
        terms_ref[u, 1] = high

    def evaluate(slot, buffer, u):
        spread_ref, terms_ref = buffer
        layer, tower_block, cell_x, cell_y, plate_block = place(slot)
        tower_rows = tower_tile(layer, tower_block) * tower_scale
        low, high = terms_ref[u, 0], terms_ref[u, 1]
        rows = [jnp.broadcast_to(tower_rows[c : c + 1], (8, lanes)) for c in range(4)]
        words = masks[slot]
        on_tower = [jnp.zeros((8, lanes), f32) for _ in range(3)]
        on_plate = [jnp.zeros((8, lanes), f32) for _ in range(3)]
        for w in range(lanes // 8):
            piece = [
                spread_ref[u, 8 * w : 8 * w + 8, lanes * c : lanes * c + lanes]
                for c in range(4)
            ]
            raw_x, raw_y, dz = (rows[c] - piece[c] for c in range(3))
            dx = raw_x - jnp.round(raw_x)
            dy = raw_y - jnp.round(raw_y)
            dist = dx * dx + ratio * (dy * dy) + dz * dz
            root = lax.rsqrt(dist + soft)
            inverse = root * root
            cube = inverse * inverse * inverse
            falloff = 1.0 - fall * dist
            word = jnp.broadcast_to(words[w : w + 1], (8, lanes))
            falloff = jnp.where(jnp.bitwise_and(word, bit) == 0, falloff, 0.0)
            falloff = jnp.maximum(falloff, 0.0) * root
            energy = cube * (high * cube - low) + rows[3] * piece[3] * root
            strength = energy * (falloff * falloff)
            for c, offset in enumerate((dx, dy, dz)):
                weighted = strength * offset
                on_tower[c] += weighted
                on_plate[c] = jnp.where(
                    lane_group == w, jnp.sum(weighted, axis=1, keepdims=True), on_plate[c]
                )
        listed = jnp.where(slot < total, 1.0, 0.0).astype(f32)
        zero = jnp.zeros((1, lanes), f32)
        tower_sum = jnp.concatenate(
            [*(jnp.sum(v, axis=0, keepdims=True) for v in on_tower), zero], axis=0
        )
        plate_sum = jnp.concatenate(
            [
                *(
                    jnp.sum(jnp.where(on_diagonal, v, 0.0), axis=0, keepdims=True)
                    for v in on_plate
                ),
                zero,
            ],
            axis=0,
        )
        factor = back * listed
        return (
            (layer, tower_block, tower_sum * factor),
            (cell_x, cell_y, plate_block, plate_sum * -factor),
        )

    def finish(done):
        for (layer, tower_block, on_tower), (cell_x, cell_y, plate_block, on_plate) in done:
            for z, ref in enumerate(tower_outs):
                ref[tower_block] += jnp.where(layer == z, on_tower, 0.0)
            for y, ref in enumerate(row_outs):
                ref[cell_x, plate_block] += jnp.where(cell_y == y, on_plate, 0.0)

    buffers = (held[0:2], held[2:4])

    def step(index, carry):
        done = []
        for half in range(2):
            first = (2 * index + half) * unroll
            for u in range(unroll):
                prepare(first + unroll + u, buffers[1 - half], u)
                done.append(evaluate(first + u, buffers[half], u))
        finish(done)
        return carry

    for u in range(unroll):
        prepare(u, buffers[0], u)
    lax.fori_loop(0, (total + 2 * unroll - 1) // (2 * unroll), step, 0)


def pair_forces(tower_list, plate_list, count, spot, tables, towers, rows, masks, lengths):
    blocks = towers[0].shape[0] - 1
    shape_one = jax.ShapeDtypeStruct((blocks, 4, lanes), jnp.float32)
    shape_row = jax.ShapeDtypeStruct((3, blocks, 4, lanes), jnp.float32)
    return pl.pallas_call(
        functools.partial(pair_kernel, *lengths, group),
        out_shape=[shape_one] * 4 + [shape_row] * 3,
        in_specs=[smem()] * 6 + [vmem()] * 8,
        out_specs=[vmem()] * 7,
        scratch_shapes=[
            pltpu.VMEM((group, lanes, 4 * lanes), jnp.float32),
            pltpu.VMEM((group, 2, 8, lanes), jnp.float32),
        ]
        * 2,
        compiler_params=pltpu.CompilerParams(vmem_limit_bytes=VMEM_LIMIT),
        cost_estimate=pl.CostEstimate(
            flops=40 * 64 * lanes * lanes, bytes_accessed=2**21, transcendentals=64 * lanes * lanes
        ),
        name="pair_forces",
    )(tower_list, plate_list, count, spot, *tables, *towers, *rows, masks)


def arrival_kernel(spot, *refs):
    first_row, own_row, second_row, out = refs
    odd_x, odd_y = spot[0], spot[1]
    for q in range(own_row.shape[1]):
        second = [second_row[k, q] for k in range(3)]
        first = [first_row[k, q] for k in range(3)]
        own = [own_row[k, q] for k in range(3)]
        for number, (x, y) in enumerate(sources):
            wanted = float((2 - x) * 3 + (2 - y))
            by_y = own
            if y != 1:
                flip = odd_y == (1 if y == 0 else 0)
                by_y = [jnp.where(flip, first[k], second[k]) for k in range(3)]
            state = by_y[1]
            if x != 1:
                flip = odd_x == (1 if x == 0 else 0)
                state = jnp.where(flip, by_y[0], by_y[2])
            kept = jnp.where(state[6:7] == wanted, state, 0.0)
            for c in range(6):
                out[c, number : number + 1, lanes * q : lanes * q + lanes] = kept[c : c + 1]


def arrivals_of(spot, rows):
    leaving = rows[0].shape[1]
    return pl.pallas_call(
        arrival_kernel,
        out_shape=jax.ShapeDtypeStruct((6, 8, leaving * lanes), jnp.float32),
        in_specs=[smem()] + [vmem()] * 3,
        out_specs=vmem(),
        compiler_params=pltpu.CompilerParams(vmem_limit_bytes=VMEM_LIMIT),
        name="arrivals",
    )(spot, *rows)


def by_block(rows):
    return rows.reshape(rows.shape[0], -1, lanes).transpose(1, 0, 2)


def by_atom(tiles):
    return tiles.transpose(1, 0, 2).reshape(tiles.shape[1], -1)


def kick_kernel(leaving, heading, features, half_kick, inv_mass, *refs):
    parts, (positions, velocities, forces, state) = refs[:-4], refs[-4:]
    blocks = half_kick.shape[0]
    for b in range(blocks):
        total = parts[0][b]
        for part in parts[1:]:
            total = total + part[b]
        force = total[0:3]
        forces[b] = force
        velocities[b] = half_kick[b] + 0.5 * time_step * force * inv_mass[b : b + 1]
        positions[b] = features[b, 0:3]
    for q in range(leaving.shape[1]):
        block = leaving[0, q]
        state[q, 0:3] = features[block, 0:3]
        state[q, 3:6] = velocities[block]
        state[q, 6:8] = jnp.full((2, lanes), heading[0, q].astype(jnp.float32))
    nothing = jnp.zeros((3, lanes), jnp.float32)
    for q in range(leaving.shape[1]):
        positions[leaving[0, q]] = nothing
        velocities[leaving[0, q]] = nothing


def kick(leaving, heading, features, half_kick, inv_mass, parts):
    blocks = half_kick.shape[0]
    shape = jax.ShapeDtypeStruct((blocks, 3, lanes), jnp.float32)
    return pl.pallas_call(
        kick_kernel,
        out_shape=[shape] * 3
        + [jax.ShapeDtypeStruct((leaving.shape[1], 8, lanes), jnp.float32)],
        in_specs=[smem()] * 2 + [vmem()] * (3 + len(parts)),
        out_specs=[vmem()] * 4,
        compiler_params=pltpu.CompilerParams(vmem_limit_bytes=VMEM_LIMIT),
        name="kick",
    )(leaving, heading, features, half_kick, inv_mass.reshape(blocks, lanes), *parts)


def local(
    positions,
    velocities,
    forces_old,
    inv_mass,
    charges,
    block_species,
    sigma_table,
    epsilon_table,
    tower_index,
    plate_index,
    tile_counts,
    exclusions,
    mig_block,
    mig_dest,
):
    layers = lax.axis_size("gz")
    length_x = float(lax.axis_size("gx"))
    length_y = float(lax.axis_size("gy"))
    half_kick = velocities + 0.5 * time_step * forces_old * inv_mass[None, :]
    moved = positions + time_step * half_kick
    kinds = block_species.astype(jnp.float32)
    kind_tile = jnp.pad(kinds[None, :], ((0, 3), (0, lanes - kinds.shape[0])))
    features = jnp.concatenate(
        [by_block(jnp.concatenate([moved, charges[None, :]])), kind_tile[None]]
    )
    me_x, me_y, me_z = (lax.axis_index(axis) for axis in ("gx", "gy", "gz"))
    spot = jnp.stack([me_x % 2, me_y % 2, me_z]).astype(jnp.int32)
    rows = halo(features)

    def from_layer(value, step):
        return lax.ppermute(value, "gz", [(i, i ^ step) for i in range(layers)])

    towers = [features] + [from_layer(features, step) for step in range(1, layers)]
    sums = pair_forces(
        tower_index,
        plate_index,
        tile_counts,
        spot,
        (sigma_table, epsilon_table),
        towers,
        rows,
        exclusions[0],
        (length_x, length_y),
    )
    parts = [sums[0]] + [from_layer(sums[step], step) for step in range(1, layers)]
    parts += sent_home(*sums[layers:])
    positions_new, velocities_new, forces_new, state = kick(
        mig_block, mig_dest, features, by_block(half_kick), inv_mass, parts
    )
    arrivals = arrivals_of(spot, halo(state))[:, None]
    return (by_atom(positions_new), by_atom(velocities_new), by_atom(forces_new), arrivals)


def solution(mesh):
    everywhere = ("gx", "gy", "gz")
    in_specs = (
        P(None, everywhere),
        P(None, everywhere),
        P(None, everywhere),
        P(everywhere),
        P(everywhere),
        P(everywhere),
        P(),
        P(),
        P(everywhere, None),
        P(everywhere, None),
        P(everywhere),
        P(everywhere, None, None, None),
        P(everywhere, None),
        P(everywhere, None),
    )
    out_specs = (
        P(None, everywhere),
        P(None, everywhere),
        P(None, everywhere),
        P(None, everywhere, None, None),
    )
    return jax.shard_map(local, mesh=mesh, in_specs=in_specs, out_specs=out_specs, check_vma=False)
```

```python
import functools

import jax
import jax.numpy as jnp
from jax import lax
from jax.experimental import pallas as pl
from jax.experimental.pallas import tpu as pltpu
from jax.sharding import PartitionSpec as P


time_step = 0.2
soft_core = 0.09
cutoff_sq = 1.44
coulomb_k = 0.5
lanes = 128
sources = ((0, 0), (0, 1), (0, 2), (1, 0), (1, 2), (2, 0), (2, 1), (2, 2))
group = 4
VMEM_LIMIT = 24 * 1024 * 1024


def pairs_first(count):
    return [(i, i + 1) for i in range(0, count, 2)]


def pairs_second(count):
    return [(i, (i + 1) % count) for i in range(1, count, 2)]


def swap(value, axis, pairs):
    return lax.ppermute(value, axis, [*pairs, *((j, i) for i, j in pairs)])


def halo(value):
    count_x, count_y = lax.axis_size("gx"), lax.axis_size("gy")
    own = jnp.stack(
        [swap(value, "gx", pairs_first(count_x)), value, swap(value, "gx", pairs_second(count_x))]
    )
    return (swap(own, "gy", pairs_first(count_y)), own, swap(own, "gy", pairs_second(count_y)))


def sent_home(first, own, second):
    count_x, count_y = lax.axis_size("gx"), lax.axis_size("gy")
    row = (
        own
        + swap(first, "gy", pairs_first(count_y))
        + swap(second, "gy", pairs_second(count_y))
    )
    return [
        row[1], swap(row[0], "gx", pairs_first(count_x)), swap(row[2], "gx", pairs_second(count_x))
    ]


def piece_of(offset, odd):
    return jnp.where(offset == 1, 1, jnp.where(offset == 2 * odd, 2, 0))


def vmem():
    return pl.BlockSpec(memory_space=pltpu.VMEM)


def smem():
    return pl.BlockSpec(memory_space=pltpu.SMEM)


def exact_parts(value):
    high = value.astype(jnp.bfloat16).astype(jnp.float32)
    rest = value - high
    middle = rest.astype(jnp.bfloat16).astype(jnp.float32)
    return high, middle, rest - middle


def pair_kernel(
    length_x,
    length_y,
    unroll,
    late,
    tower_list,
    plate_list,
    count,
    spot,
    sigma_table,
    epsilon_table,
    *refs,
):
    count_rows = 1 if late else 2
    tower_refs, plate_rows_held, refs = refs[0:4], refs[4 : 4 + count_rows], refs[4 + count_rows :]
    masks, refs = refs[0], refs[1:]
    if late:
        earlier, refs = refs[0:4], refs[4:]
    tower_outs, row_outs, held = refs[0:4], refs[4 : 4 + count_rows], refs[4 + count_rows : -1]
    listed_slots = refs[-1]
    blocks = tower_outs[0].shape[0]
    for z, ref in enumerate(tower_outs):
        ref[...] = earlier[z][...] if late else jnp.zeros_like(ref)
    for ref in row_outs:
        ref[...] = jnp.zeros_like(ref)
    odd_x, odd_y, me_z = (spot[n] for n in range(3))
    f32 = jnp.float32
    row4 = lax.broadcasted_iota(jnp.int32, (4, lanes), 0)
    lane4 = lax.broadcasted_iota(jnp.int32, (4, lanes), 1)
    sub = lax.broadcasted_iota(jnp.int32, (8, lanes), 0)
    lane = lax.broadcasted_iota(jnp.int32, (8, lanes), 1)
    lane_group = lane // 8
    on_diagonal = sub == lane % 8
    bit = jnp.left_shift(jnp.int32(1), sub)
    scale = jnp.where(
        row4 == 0,
        1.0 / length_x,
        jnp.where(row4 == 1, 1.0 / length_y, jnp.where(row4 == 2, 1.0 / length_x, 1.0)),
    ).astype(f32)
    ratio = (length_y / length_x) ** 2
    unit_sq = length_x * length_x
    soft = soft_core / unit_sq
    fall = unit_sq / cutoff_sq
    tower_scale = jnp.where(row4 == 3, coulomb_k / length_x, scale).astype(f32)
    back = jnp.where(
        row4 == 0,
        length_x / unit_sq,
        jnp.where(row4 == 1, length_y / unit_sq, length_x / unit_sq),
    ).astype(f32)
    pick = jnp.concatenate(
        [
            jnp.where(
                jnp.logical_and(
                    lax.broadcasted_iota(jnp.int32, (16, lanes), 0) % 4 == c,
                    lax.broadcasted_iota(jnp.int32, (16, lanes), 0) < 12,
                ),
                1.0,
                0.0,
            ).astype(f32)
            for c in range(4)
        ],
        axis=1,
    ).astype(jnp.bfloat16)
    all_slots = count[0]
    sigmas = [jnp.full((1, 1), sigma_table[n]) for n in range(sigma_table.shape[0])]
    depths = [jnp.sqrt(jnp.full((1, 1), epsilon_table[n])) for n in range(sigma_table.shape[0])]

    def of_kind(table, kind):
        value = table[0]
        for n in range(1, len(table)):
            value = jnp.where(kind == n, table[n], value)
        return value


    shift = blocks.bit_length() - 1

    def place(slot):
        tower, plate = tower_list[0, slot], plate_list[0, slot]
        cell = jnp.right_shift(plate, shift)
        cell_x = jnp.right_shift(cell * 11, 5)
        return (
            jnp.bitwise_xor(jnp.right_shift(tower, shift), me_z),
            jnp.bitwise_and(tower, blocks - 1),
            piece_of(cell_x, odd_x),
            piece_of(cell - 3 * cell_x, odd_y),
            jnp.bitwise_and(plate, blocks - 1),
        )

    def tower_tile(layer, row):
        near = jnp.where(layer == 0, tower_refs[0][row], tower_refs[1][row])
        return jnp.where(
            layer < 2, near, jnp.where(layer == 2, tower_refs[2][row], tower_refs[3][row])
        )

    spare = listed_slots.shape[0]
    late_row = 2 * odd_y

    def gather(step, found):
        for u in range(8):
            slot = 8 * step + u
            cell = jnp.right_shift(plate_list[0, slot], shift)
            is_late = (cell - 3 * jnp.right_shift(cell * 11, 5) == late_row).astype(jnp.int32)
            listed_slots[found] = slot
            found = found + jnp.where(slot < all_slots, is_late if late else 1 - is_late, 0)
        return found

    total = lax.fori_loop(0, tower_list.shape[1] // 8, gather, 0)

    def slot_at(number):
        slot = listed_slots[jnp.minimum(number, spare - 1)]
        return jnp.where(number < total, slot, 0)


    def prepare(slot, buffer, u):
        spread_ref, terms_ref = buffer
        layer, tower_block, cell_x, cell_y, plate_block = place(slot_at(slot))
        tower_kind = tower_tile(layer, blocks)

        def chosen(row):
            found = [ref[cell_x, row] for ref in plate_rows_held]
            return found[0] if late else jnp.where(cell_y == 0, found[0], found[1])

        plate_rows = chosen(plate_block) * scale
        plate_kind = chosen(blocks)
        of_tower = jnp.sum(
            jnp.where(lane4 == tower_block, tower_kind, 0.0), axis=1, keepdims=True
        )
        of_plate = jnp.sum(
            jnp.where(lane4 == plate_block, plate_kind, 0.0), axis=1, keepdims=True
        )
        kind_one, kind_two = of_tower[0:1], of_plate[0:1]
        sigma = 0.5 * (of_kind(sigmas, kind_one) + of_kind(sigmas, kind_two))
        depth = of_kind(depths, kind_one) * of_kind(depths, kind_two)
        sigma_sq = sigma * sigma * (1.0 / unit_sq)
        sigma_six = sigma_sq * sigma_sq * sigma_sq
        low = jnp.broadcast_to(6.0 * depth * sigma_six, (8, lanes))
        high = jnp.broadcast_to(12.0 * depth * sigma_six * sigma_six, (8, lanes))
        parts = jnp.concatenate([*exact_parts(plate_rows), jnp.zeros_like(plate_rows)], axis=0)
        spread_ref[u] = lax.dot_general(
            parts.astype(jnp.bfloat16),
            pick,
            (((0,), (0,)), ((), ())),
            preferred_element_type=f32,
        )
        terms_ref[u, 0] = low
        terms_ref[u, 1] = high

    def evaluate(slot, buffer, u):
        spread_ref, terms_ref = buffer
        layer, tower_block, cell_x, cell_y, plate_block = place(slot_at(slot))
        tower_rows = tower_tile(layer, tower_block) * tower_scale
        low, high = terms_ref[u, 0], terms_ref[u, 1]
        rows = [jnp.broadcast_to(tower_rows[c : c + 1], (8, lanes)) for c in range(4)]
        words = masks[slot_at(slot)]
        on_tower = [jnp.zeros((8, lanes), f32) for _ in range(3)]
        on_plate = [jnp.zeros((8, lanes), f32) for _ in range(3)]
        for w in range(lanes // 8):
            piece = [
                spread_ref[u, 8 * w : 8 * w + 8, lanes * c : lanes * c + lanes]
                for c in range(4)
            ]
            raw_x, raw_y, dz = (rows[c] - piece[c] for c in range(3))
            dx = raw_x - jnp.round(raw_x)
            dy = raw_y - jnp.round(raw_y)
            dist = dx * dx + ratio * (dy * dy) + dz * dz
            root = lax.rsqrt(dist + soft)
            inverse = root * root
            cube = inverse * inverse * inverse
            falloff = 1.0 - fall * dist
            word = jnp.broadcast_to(words[w : w + 1], (8, lanes))
            falloff = jnp.where(jnp.bitwise_and(word, bit) == 0, falloff, 0.0)
            falloff = jnp.maximum(falloff, 0.0) * root
            energy = cube * (high * cube - low) + rows[3] * piece[3] * root
            strength = energy * (falloff * falloff)
            for c, offset in enumerate((dx, dy, dz)):
                weighted = strength * offset
                on_tower[c] += weighted
                on_plate[c] = jnp.where(
                    lane_group == w, jnp.sum(weighted, axis=1, keepdims=True), on_plate[c]
                )
        listed = jnp.where(slot < total, 1.0, 0.0).astype(f32)
        zero = jnp.zeros((1, lanes), f32)
        tower_sum = jnp.concatenate(
            [*(jnp.sum(v, axis=0, keepdims=True) for v in on_tower), zero], axis=0
        )
        plate_sum = jnp.concatenate(
            [
                *(
                    jnp.sum(jnp.where(on_diagonal, v, 0.0), axis=0, keepdims=True)
                    for v in on_plate
                ),
                zero,
            ],
            axis=0,
        )
        factor = back * listed
        return (
            (layer, tower_block, tower_sum * factor),
            (cell_x, cell_y, plate_block, plate_sum * -factor),
        )

    def finish(done):
        for (layer, tower_block, on_tower), (cell_x, cell_y, plate_block, on_plate) in done:
            for z, ref in enumerate(tower_outs):
                ref[tower_block] += jnp.where(layer == z, on_tower, 0.0)
            for y, ref in enumerate(row_outs):
                ref[cell_x, plate_block] += (
                    on_plate if late else jnp.where(cell_y == y, on_plate, 0.0)
                )

    buffers = (held[0:2], held[2:4])

    def step(index, carry):
        done = []
        for half in range(2):
            first = (2 * index + half) * unroll
            for u in range(unroll):
                prepare(first + unroll + u, buffers[1 - half], u)
                done.append(evaluate(first + u, buffers[half], u))
        finish(done)
        return carry

    for u in range(unroll):
        prepare(u, buffers[0], u)
    lax.fori_loop(0, (total + 2 * unroll - 1) // (2 * unroll), step, 0)


def pair_forces(lists, spot, tables, towers, rows, masks, lengths, earlier=()):
    late = len(earlier) > 0
    blocks = towers[0].shape[0] - 1
    slots = lists[0].shape[1]
    shape_one = jax.ShapeDtypeStruct((blocks, 4, lanes), jnp.float32)
    shape_row = jax.ShapeDtypeStruct((3, blocks, 4, lanes), jnp.float32)
    flops = 20 * slots * lanes * lanes
    size = 2 if late else group
    return pl.pallas_call(
        functools.partial(pair_kernel, *lengths, size, late),
        out_shape=[shape_one] * 4 + [shape_row] * len(rows),
        in_specs=[smem()] * 6 + [vmem()] * (5 + len(rows) + len(earlier)),
        out_specs=[vmem()] * (4 + len(rows)),
        scratch_shapes=[
            pltpu.VMEM((size, lanes, 4 * lanes), jnp.float32),
            pltpu.VMEM((size, 2, 8, lanes), jnp.float32),
        ]
        * 2
        + [pltpu.SMEM((slots + 1,), jnp.int32)],
        compiler_params=pltpu.CompilerParams(vmem_limit_bytes=VMEM_LIMIT),
        cost_estimate=pl.CostEstimate(
            flops=flops, bytes_accessed=2**20, transcendentals=flops // 40
        ),
        name="pairs_late" if late else "pairs_early",
    )(*lists, spot, *tables, *towers, *rows, masks, *earlier)


def arrival_kernel(spot, *refs):
    first_row, own_row, second_row, out = refs
    odd_x, odd_y = spot[0], spot[1]
    for q in range(own_row.shape[1]):
        second = [second_row[k, q] for k in range(3)]
        first = [first_row[k, q] for k in range(3)]
        own = [own_row[k, q] for k in range(3)]
        for number, (x, y) in enumerate(sources):
            wanted = float((2 - x) * 3 + (2 - y))
            by_y = own
            if y != 1:
                flip = odd_y == (1 if y == 0 else 0)
                by_y = [jnp.where(flip, first[k], second[k]) for k in range(3)]
            state = by_y[1]
            if x != 1:
                flip = odd_x == (1 if x == 0 else 0)
                state = jnp.where(flip, by_y[0], by_y[2])
            kept = jnp.where(state[6:7] == wanted, state, 0.0)
            for c in range(6):
                out[c, number : number + 1, lanes * q : lanes * q + lanes] = kept[c : c + 1]


def arrivals_of(spot, rows):
    leaving = rows[0].shape[1]
    return pl.pallas_call(
        arrival_kernel,
        out_shape=jax.ShapeDtypeStruct((6, 8, leaving * lanes), jnp.float32),
        in_specs=[smem()] + [vmem()] * 3,
        out_specs=vmem(),
        compiler_params=pltpu.CompilerParams(vmem_limit_bytes=VMEM_LIMIT),
        name="arrivals",
    )(spot, *rows)


def by_block(rows):
    return rows.reshape(rows.shape[0], -1, lanes).transpose(1, 0, 2)


def by_atom(tiles):
    return tiles.transpose(1, 0, 2).reshape(tiles.shape[1], -1)


def kick_kernel(spot, features, half_kick, inv_mass, *refs):
    parts, (positions, velocities, forces, state) = refs[:-4], refs[-4:]
    count = state.shape[0]
    leaving = [spot[3 + q] for q in range(count)]
    heading = [spot[3 + count + q] for q in range(count)]
    blocks = half_kick.shape[0]
    for b in range(blocks):
        total = parts[0][b]
        for part in parts[1:]:
            total = total + part[b]
        force = total[0:3]
        forces[b] = force
        velocities[b] = half_kick[b] + 0.5 * time_step * force * inv_mass[b : b + 1]
        positions[b] = features[b, 0:3]
    for q in range(count):
        block = leaving[q]
        state[q, 0:3] = features[block, 0:3]
        state[q, 3:6] = velocities[block]
        state[q, 6:8] = jnp.full((2, lanes), heading[q].astype(jnp.float32))
    nothing = jnp.zeros((3, lanes), jnp.float32)
    for q in range(count):
        positions[leaving[q]] = nothing
        velocities[leaving[q]] = nothing


def kick(spot, count, features, half_kick, inv_mass, parts):
    blocks = half_kick.shape[0]
    shape = jax.ShapeDtypeStruct((blocks, 3, lanes), jnp.float32)
    return pl.pallas_call(
        kick_kernel,
        out_shape=[shape] * 3
        + [jax.ShapeDtypeStruct((count, 8, lanes), jnp.float32)],
        in_specs=[smem()] + [vmem()] * (3 + len(parts)),
        out_specs=[vmem()] * 4,
        compiler_params=pltpu.CompilerParams(vmem_limit_bytes=VMEM_LIMIT),
        name="kick",
    )(spot, features, half_kick, inv_mass.reshape(blocks, lanes), *parts)


def local(
    positions,
    velocities,
    forces_old,
    inv_mass,
    charges,
    block_species,
    sigma_table,
    epsilon_table,
    tower_index,
    plate_index,
    tile_counts,
    exclusions,
    mig_block,
    mig_dest,
):
    layers = lax.axis_size("gz")
    length_x = float(lax.axis_size("gx"))
    length_y = float(lax.axis_size("gy"))
    half_kick = velocities + 0.5 * time_step * forces_old * inv_mass[None, :]
    moved = positions + time_step * half_kick
    kinds = block_species.astype(jnp.float32)
    kind_tile = jnp.pad(kinds[None, :], ((0, 3), (0, lanes - kinds.shape[0])))
    features = jnp.concatenate(
        [by_block(jnp.concatenate([moved, charges[None, :]])), kind_tile[None]]
    )
    me_x, me_y, me_z = (lax.axis_index(axis) for axis in ("gx", "gy", "gz"))
    spot = jnp.stack([me_x % 2, me_y % 2, me_z]).astype(jnp.int32)
    spot = jnp.concatenate([spot, mig_block[0], mig_dest[0]])
    rows = halo(features)

    def from_layer(value, step):
        return lax.ppermute(value, "gz", [(i, i ^ step) for i in range(layers)])

    towers = [features] + [from_layer(features, step) for step in range(1, layers)]
    first, own, second = rows

    def pairs(rows, earlier=()):
        return pair_forces(
            (tower_index, plate_index, tile_counts),
            spot,
            (sigma_table, epsilon_table),
            towers,
            rows,
            exclusions[0],
            (length_x, length_y),
            earlier,
        )

    *early, on_first, on_own = pairs((first, own))
    *sums, on_second = pairs((second,), early)
    parts = [sums[0]] + [from_layer(sums[step], step) for step in range(1, layers)]
    parts += sent_home(on_first, on_own, on_second)
    positions_new, velocities_new, forces_new, state = kick(
        spot, mig_block.shape[1], features, by_block(half_kick), inv_mass, parts
    )
    arrivals = arrivals_of(spot, halo(state))[:, None]
    return (by_atom(positions_new), by_atom(velocities_new), by_atom(forces_new), arrivals)


def solution(mesh):
    everywhere = ("gx", "gy", "gz")
    in_specs = (
        P(None, everywhere),
        P(None, everywhere),
        P(None, everywhere),
        P(everywhere),
        P(everywhere),
        P(everywhere),
        P(),
        P(),
        P(everywhere, None),
        P(everywhere, None),
        P(everywhere),
        P(everywhere, None, None, None),
        P(everywhere, None),
        P(everywhere, None),
    )
    out_specs = (
        P(None, everywhere),
        P(None, everywhere),
        P(None, everywhere),
        P(None, everywhere, None, None),
    )
    return jax.shard_map(local, mesh=mesh, in_specs=in_specs, out_specs=out_specs, check_vma=False)
```

```python
import functools

import jax
import jax.numpy as jnp
from jax import lax
from jax.experimental import pallas as pl
from jax.experimental.pallas import tpu as pltpu
from jax.sharding import PartitionSpec as P


time_step = 0.2
soft_core = 0.09
cutoff_sq = 1.44
coulomb_k = 0.5
lanes = 128
sources = ((0, 0), (0, 1), (0, 2), (1, 0), (1, 2), (2, 0), (2, 1), (2, 2))
group = 4
VMEM_LIMIT = 24 * 1024 * 1024


def pairs_first(count):
    return [(i, i + 1) for i in range(0, count, 2)]


def pairs_second(count):
    return [(i, (i + 1) % count) for i in range(1, count, 2)]


def swap(value, axis, pairs):
    return lax.ppermute(value, axis, [*pairs, *((j, i) for i, j in pairs)])


def halo(value):
    count_x, count_y = lax.axis_size("gx"), lax.axis_size("gy")
    own = jnp.stack(
        [swap(value, "gx", pairs_first(count_x)), value, swap(value, "gx", pairs_second(count_x))]
    )
    return (swap(own, "gy", pairs_first(count_y)), own, swap(own, "gy", pairs_second(count_y)))


def sum_kernel(own, first, second, *outs):
    for x, out in enumerate(outs):
        for b in range(out.shape[0]):
            out[b] = own[x, b] + first[x, b]
        for c in range(3):
            for b in range(out.shape[0]):
                out[b, c : c + 1] += second[x, c, b : b + 1]


def row_sums(own, first, second):
    return pl.pallas_call(
        sum_kernel,
        out_shape=[jax.ShapeDtypeStruct(own.shape[1:], jnp.float32)] * 3,
        in_specs=[vmem()] * 3,
        out_specs=[vmem()] * 3,
        compiler_params=pltpu.CompilerParams(vmem_limit_bytes=VMEM_LIMIT),
        name="row_sums",
    )(own, first, second)


def sent_home(first, own, second):
    count_x, count_y = lax.axis_size("gx"), lax.axis_size("gy")
    row = row_sums(
        own, swap(first, "gy", pairs_first(count_y)), swap(second, "gy", pairs_second(count_y))
    )
    return [
        row[1], swap(row[0], "gx", pairs_first(count_x)), swap(row[2], "gx", pairs_second(count_x))
    ]


def piece_of(offset, odd):
    return jnp.where(offset == 1, 1, jnp.where(offset == 2 * odd, 2, 0))


def vmem():
    return pl.BlockSpec(memory_space=pltpu.VMEM)


def smem():
    return pl.BlockSpec(memory_space=pltpu.SMEM)


def exact_parts(value):
    high = value.astype(jnp.bfloat16).astype(jnp.float32)
    rest = value - high
    middle = rest.astype(jnp.bfloat16).astype(jnp.float32)
    return high, middle, rest - middle


def pair_kernel(
    length_x,
    length_y,
    unroll,
    late,
    tower_list,
    plate_list,
    count,
    spot,
    sigma_table,
    epsilon_table,
    *refs,
):
    count_rows = 1 if late else 2
    tower_refs, plate_rows_held, refs = refs[0:4], refs[4 : 4 + count_rows], refs[4 + count_rows :]
    masks, refs = refs[0], refs[1:]
    if late:
        earlier, refs = refs[0:4], refs[4:]
    tower_outs, row_outs, held = refs[0:4], refs[4 : 4 + count_rows], refs[4 + count_rows : -1]
    listed_slots = refs[-1]
    blocks = tower_outs[0].shape[0]
    for z, ref in enumerate(tower_outs):
        ref[...] = earlier[z][...] if late else jnp.zeros_like(ref)
    for ref in row_outs:
        ref[...] = jnp.zeros_like(ref)
    odd_x, odd_y, me_z = (spot[n] for n in range(3))
    f32 = jnp.float32
    row4 = lax.broadcasted_iota(jnp.int32, (4, lanes), 0)
    lane4 = lax.broadcasted_iota(jnp.int32, (4, lanes), 1)
    sub = lax.broadcasted_iota(jnp.int32, (8, lanes), 0)
    lane = lax.broadcasted_iota(jnp.int32, (8, lanes), 1)
    lane_group = lane // 8
    on_diagonal = sub == lane % 8
    bit = jnp.left_shift(jnp.int32(1), sub)
    scale = jnp.where(
        row4 == 0,
        1.0 / length_x,
        jnp.where(row4 == 1, 1.0 / length_y, jnp.where(row4 == 2, 1.0 / length_x, 1.0)),
    ).astype(f32)
    ratio = (length_y / length_x) ** 2
    unit_sq = length_x * length_x
    soft = soft_core / unit_sq
    fall = unit_sq / cutoff_sq
    tower_scale = jnp.where(row4 == 3, coulomb_k / length_x, scale).astype(f32)
    back = jnp.where(
        row4 == 0,
        length_x / unit_sq,
        jnp.where(row4 == 1, length_y / unit_sq, length_x / unit_sq),
    ).astype(f32)
    pick = jnp.concatenate(
        [
            jnp.where(
                jnp.logical_and(
                    lax.broadcasted_iota(jnp.int32, (16, lanes), 0) % 4 == c,
                    lax.broadcasted_iota(jnp.int32, (16, lanes), 0) < 12,
                ),
                1.0,
                0.0,
            ).astype(f32)
            for c in range(4)
        ],
        axis=1,
    ).astype(jnp.bfloat16)
    all_slots = count[0]
    sigmas = [jnp.full((1, 1), sigma_table[n]) for n in range(sigma_table.shape[0])]
    depths = [jnp.sqrt(jnp.full((1, 1), epsilon_table[n])) for n in range(sigma_table.shape[0])]

    def of_kind(table, kind):
        value = table[0]
        for n in range(1, len(table)):
            value = jnp.where(kind == n, table[n], value)
        return value


    shift = blocks.bit_length() - 1

    def place(slot):
        tower, plate = tower_list[0, slot], plate_list[0, slot]
        cell = jnp.right_shift(plate, shift)
        cell_x = jnp.right_shift(cell * 11, 5)
        return (
            jnp.bitwise_xor(jnp.right_shift(tower, shift), me_z),
            jnp.bitwise_and(tower, blocks - 1),
            piece_of(cell_x, odd_x),
            piece_of(cell - 3 * cell_x, odd_y),
            jnp.bitwise_and(plate, blocks - 1),
        )

    def tower_tile(layer, row):
        near = jnp.where(layer == 0, tower_refs[0][row], tower_refs[1][row])
        return jnp.where(
            layer < 2, near, jnp.where(layer == 2, tower_refs[2][row], tower_refs[3][row])
        )

    spare = listed_slots.shape[0]
    late_row = 2 * odd_y

    def gather(step, found):
        for u in range(8):
            slot = 8 * step + u
            cell = jnp.right_shift(plate_list[0, slot], shift)
            is_late = (cell - 3 * jnp.right_shift(cell * 11, 5) == late_row).astype(jnp.int32)
            listed_slots[found] = slot
            found = found + jnp.where(slot < all_slots, is_late if late else 1 - is_late, 0)
        return found

    total = lax.fori_loop(0, tower_list.shape[1] // 8, gather, 0)

    def slot_at(number):
        slot = listed_slots[jnp.minimum(number, spare - 1)]
        return jnp.where(number < total, slot, 0)


    def prepare(slot, buffer, u):
        spread_ref, terms_ref = buffer
        layer, tower_block, cell_x, cell_y, plate_block = place(slot_at(slot))
        tower_kind = tower_tile(layer, blocks)

        def chosen(row):
            found = [ref[cell_x, row] for ref in plate_rows_held]
            return found[0] if late else jnp.where(cell_y == 0, found[0], found[1])

        plate_rows = chosen(plate_block) * scale
        plate_kind = chosen(blocks)
        of_tower = jnp.sum(
            jnp.where(lane4 == tower_block, tower_kind, 0.0), axis=1, keepdims=True
        )
        of_plate = jnp.sum(
            jnp.where(lane4 == plate_block, plate_kind, 0.0), axis=1, keepdims=True
        )
        kind_one, kind_two = of_tower[0:1], of_plate[0:1]
        sigma = 0.5 * (of_kind(sigmas, kind_one) + of_kind(sigmas, kind_two))
        depth = of_kind(depths, kind_one) * of_kind(depths, kind_two)
        sigma_sq = sigma * sigma * (1.0 / unit_sq)
        sigma_six = sigma_sq * sigma_sq * sigma_sq
        low = jnp.broadcast_to(6.0 * depth * sigma_six, (8, lanes))
        high = jnp.broadcast_to(12.0 * depth * sigma_six * sigma_six, (8, lanes))
        parts = jnp.concatenate([*exact_parts(plate_rows), jnp.zeros_like(plate_rows)], axis=0)
        spread_ref[u] = lax.dot_general(
            parts.astype(jnp.bfloat16),
            pick,
            (((0,), (0,)), ((), ())),
            preferred_element_type=f32,
        )
        terms_ref[u, 0] = low
        terms_ref[u, 1] = high

    def evaluate(slot, buffer, u):
        spread_ref, terms_ref = buffer
        layer, tower_block, cell_x, cell_y, plate_block = place(slot_at(slot))
        tower_rows = tower_tile(layer, tower_block) * tower_scale
        low, high = terms_ref[u, 0], terms_ref[u, 1]
        rows = [jnp.broadcast_to(tower_rows[c : c + 1], (8, lanes)) for c in range(4)]
        words = masks[slot_at(slot)]
        on_tower = [jnp.zeros((8, lanes), f32) for _ in range(3)]
        on_plate = [jnp.zeros((8, lanes), f32) for _ in range(3)]
        for w in range(lanes // 8):
            piece = [
                spread_ref[u, 8 * w : 8 * w + 8, lanes * c : lanes * c + lanes]
                for c in range(4)
            ]
            raw_x, raw_y, dz = (rows[c] - piece[c] for c in range(3))
            dx = raw_x - jnp.round(raw_x)
            dy = raw_y - jnp.round(raw_y)
            dist = dx * dx + ratio * (dy * dy) + dz * dz
            root = lax.rsqrt(dist + soft)
            inverse = root * root
            cube = inverse * inverse * inverse
            falloff = 1.0 - fall * dist
            word = jnp.broadcast_to(words[w : w + 1], (8, lanes))
            falloff = jnp.where(jnp.bitwise_and(word, bit) == 0, falloff, 0.0)
            falloff = jnp.maximum(falloff, 0.0) * root
            energy = cube * (high * cube - low) + rows[3] * piece[3] * root
            strength = energy * (falloff * falloff)
            for c, offset in enumerate((dx, dy, dz)):
                weighted = strength * offset
                on_tower[c] += weighted
                on_plate[c] = jnp.where(
                    lane_group == w, jnp.sum(weighted, axis=1, keepdims=True), on_plate[c]
                )
        listed = jnp.where(slot < total, 1.0, 0.0).astype(f32)
        zero = jnp.zeros((1, lanes), f32)
        tower_sum = jnp.concatenate(
            [*(jnp.sum(v, axis=0, keepdims=True) for v in on_tower), zero], axis=0
        )
        plate_sum = jnp.concatenate(
            [
                *(
                    jnp.sum(jnp.where(on_diagonal, v, 0.0), axis=0, keepdims=True)
                    for v in on_plate
                ),
                zero,
            ],
            axis=0,
        )
        factor = back * listed
        return (
            (layer, tower_block, tower_sum * factor),
            (cell_x, cell_y, plate_block, plate_sum * -factor),
        )

    def finish(done):
        for (layer, tower_block, on_tower), (cell_x, cell_y, plate_block, on_plate) in done:
            for z, ref in enumerate(tower_outs):
                ref[tower_block] += jnp.where(layer == z, on_tower, 0.0)
            for y, ref in enumerate(row_outs):
                if late:
                    place_in = pl.ds(plate_block, 1)
                    for c in range(3):
                        ref[cell_x, c, place_in, :] += on_plate[c : c + 1]
                else:
                    ref[cell_x, plate_block] += jnp.where(cell_y == y, on_plate, 0.0)

    buffers = (held[0:2], held[2:4])

    def step(index, carry):
        done = []
        for half in range(2):
            first = (2 * index + half) * unroll
            for u in range(unroll):
                prepare(first + unroll + u, buffers[1 - half], u)
                done.append(evaluate(first + u, buffers[half], u))
        finish(done)
        return carry

    for u in range(unroll):
        prepare(u, buffers[0], u)
    lax.fori_loop(0, (total + 2 * unroll - 1) // (2 * unroll), step, 0)


def pair_forces(lists, spot, tables, towers, rows, masks, lengths, earlier=()):
    late = len(earlier) > 0
    blocks = towers[0].shape[0] - 1
    slots = lists[0].shape[1]
    shape_one = jax.ShapeDtypeStruct((blocks, 4, lanes), jnp.float32)
    dims_row = (3, 3, blocks, lanes) if late else (3, blocks, 4, lanes)
    shape_row = jax.ShapeDtypeStruct(dims_row, jnp.float32)
    flops = 20 * slots * lanes * lanes
    size = 2 if late else group
    return pl.pallas_call(
        functools.partial(pair_kernel, *lengths, size, late),
        out_shape=[shape_one] * 4 + [shape_row] * len(rows),
        in_specs=[smem()] * 6 + [vmem()] * (5 + len(rows) + len(earlier)),
        out_specs=[vmem()] * (4 + len(rows)),
        scratch_shapes=[
            pltpu.VMEM((size, lanes, 4 * lanes), jnp.float32),
            pltpu.VMEM((size, 2, 8, lanes), jnp.float32),
        ]
        * 2
        + [pltpu.SMEM((slots + 1,), jnp.int32)],
        compiler_params=pltpu.CompilerParams(vmem_limit_bytes=VMEM_LIMIT),
        cost_estimate=pl.CostEstimate(
            flops=flops, bytes_accessed=2**20, transcendentals=flops // 40
        ),
        name="pairs_late" if late else "pairs_early",
    )(*lists, spot, *tables, *towers, *rows, masks, *earlier)


def arrival_kernel(spot, *refs):
    first_row, own_row, second_row, out = refs
    odd_x, odd_y = spot[0], spot[1]
    for q in range(own_row.shape[1]):
        second = [second_row[k, q] for k in range(3)]
        first = [first_row[k, q] for k in range(3)]
        own = [own_row[k, q] for k in range(3)]
        for number, (x, y) in enumerate(sources):
            wanted = float((2 - x) * 3 + (2 - y))
            by_y = own
            if y != 1:
                flip = odd_y == (1 if y == 0 else 0)
                by_y = [jnp.where(flip, first[k], second[k]) for k in range(3)]
            state = by_y[1]
            if x != 1:
                flip = odd_x == (1 if x == 0 else 0)
                state = jnp.where(flip, by_y[0], by_y[2])
            kept = jnp.where(state[6:7] == wanted, state, 0.0)
            for c in range(6):
                out[c, number : number + 1, lanes * q : lanes * q + lanes] = kept[c : c + 1]


def arrivals_of(spot, rows):
    leaving = rows[0].shape[1]
    return pl.pallas_call(
        arrival_kernel,
        out_shape=jax.ShapeDtypeStruct((6, 8, leaving * lanes), jnp.float32),
        in_specs=[smem()] + [vmem()] * 3,
        out_specs=vmem(),
        compiler_params=pltpu.CompilerParams(vmem_limit_bytes=VMEM_LIMIT),
        name="arrivals",
    )(spot, *rows)


def by_block(rows):
    return rows.reshape(rows.shape[0], -1, lanes).transpose(1, 0, 2)


def by_atom(tiles):
    return tiles.transpose(1, 0, 2).reshape(tiles.shape[1], -1)


def kick_kernel(spot, features, half_kick, inv_mass, *refs):
    parts, (positions, velocities, forces, state) = refs[:-4], refs[-4:]
    count = state.shape[0]
    leaving = [spot[3 + q] for q in range(count)]
    heading = [spot[3 + count + q] for q in range(count)]
    blocks = half_kick.shape[0]
    for b in range(blocks):
        total = parts[0][b]
        for part in parts[1:]:
            total = total + part[b]
        force = total[0:3]
        forces[b] = force
        velocities[b] = half_kick[b] + 0.5 * time_step * force * inv_mass[b : b + 1]
        positions[b] = features[b, 0:3]
    for q in range(count):
        block = leaving[q]
        state[q, 0:3] = features[block, 0:3]
        state[q, 3:6] = velocities[block]
        state[q, 6:8] = jnp.full((2, lanes), heading[q].astype(jnp.float32))
    nothing = jnp.zeros((3, lanes), jnp.float32)
    for q in range(count):
        positions[leaving[q]] = nothing
        velocities[leaving[q]] = nothing


def kick(spot, count, features, half_kick, inv_mass, parts):
    blocks = half_kick.shape[0]
    shape = jax.ShapeDtypeStruct((blocks, 3, lanes), jnp.float32)
    return pl.pallas_call(
        kick_kernel,
        out_shape=[shape] * 3
        + [jax.ShapeDtypeStruct((count, 8, lanes), jnp.float32)],
        in_specs=[smem()] + [vmem()] * (3 + len(parts)),
        out_specs=[vmem()] * 4,
        compiler_params=pltpu.CompilerParams(vmem_limit_bytes=VMEM_LIMIT),
        name="kick",
    )(spot, features, half_kick, inv_mass.reshape(blocks, lanes), *parts)


def local(
    positions,
    velocities,
    forces_old,
    inv_mass,
    charges,
    block_species,
    sigma_table,
    epsilon_table,
    tower_index,
    plate_index,
    tile_counts,
    exclusions,
    mig_block,
    mig_dest,
):
    layers = lax.axis_size("gz")
    length_x = float(lax.axis_size("gx"))
    length_y = float(lax.axis_size("gy"))
    half_kick = velocities + 0.5 * time_step * forces_old * inv_mass[None, :]
    moved = positions + time_step * half_kick
    kinds = block_species.astype(jnp.float32)
    kind_tile = jnp.pad(kinds[None, :], ((0, 3), (0, lanes - kinds.shape[0])))
    features = jnp.concatenate(
        [by_block(jnp.concatenate([moved, charges[None, :]])), kind_tile[None]]
    )
    me_x, me_y, me_z = (lax.axis_index(axis) for axis in ("gx", "gy", "gz"))
    spot = jnp.stack([me_x % 2, me_y % 2, me_z]).astype(jnp.int32)
    spot = jnp.concatenate([spot, mig_block[0], mig_dest[0]])
    rows = halo(features)

    def from_layer(value, step):
        return lax.ppermute(value, "gz", [(i, i ^ step) for i in range(layers)])

    towers = [features] + [from_layer(features, step) for step in range(1, layers)]
    first, own, second = rows

    def pairs(rows, earlier=()):
        return pair_forces(
            (tower_index, plate_index, tile_counts),
            spot,
            (sigma_table, epsilon_table),
            towers,
            rows,
            exclusions[0],
            (length_x, length_y),
            earlier,
        )

    *early, on_first, on_own = pairs((first, own))
    *sums, on_second = pairs((second,), early)
    parts = [sums[0]] + [from_layer(sums[step], step) for step in range(1, layers)]
    parts += sent_home(on_first, on_own, on_second)
    positions_new, velocities_new, forces_new, state = kick(
        spot, mig_block.shape[1], features, by_block(half_kick), inv_mass, parts
    )
    arrivals = arrivals_of(spot, halo(state))[:, None]
    return (by_atom(positions_new), by_atom(velocities_new), by_atom(forces_new), arrivals)


def solution(mesh):
    everywhere = ("gx", "gy", "gz")
    in_specs = (
        P(None, everywhere),
        P(None, everywhere),
        P(None, everywhere),
        P(everywhere),
        P(everywhere),
        P(everywhere),
        P(),
        P(),
        P(everywhere, None),
        P(everywhere, None),
        P(everywhere),
        P(everywhere, None, None, None),
        P(everywhere, None),
        P(everywhere, None),
    )
    out_specs = (
        P(None, everywhere),
        P(None, everywhere),
        P(None, everywhere),
        P(None, everywhere, None, None),
    )
    return jax.shard_map(local, mesh=mesh, in_specs=in_specs, out_specs=out_specs, check_vma=False)
```

```python
import functools

import jax
import jax.numpy as jnp
from jax import lax
from jax.experimental import pallas as pl
from jax.experimental.pallas import tpu as pltpu
from jax.sharding import PartitionSpec as P


time_step = 0.2
soft_core = 0.09
cutoff_sq = 1.44
coulomb_k = 0.5
lanes = 128
sources = ((0, 0), (0, 1), (0, 2), (1, 0), (1, 2), (2, 0), (2, 1), (2, 2))
group = 4
VMEM_LIMIT = 24 * 1024 * 1024


def pairs_first(count):
    return [(i, i + 1) for i in range(0, count, 2)]


def pairs_second(count):
    return [(i, (i + 1) % count) for i in range(1, count, 2)]


def swap(value, axis, pairs):
    return lax.ppermute(value, axis, [*pairs, *((j, i) for i, j in pairs)])


def halo(value):
    count_x, count_y = lax.axis_size("gx"), lax.axis_size("gy")
    own = jnp.stack(
        [swap(value, "gx", pairs_first(count_x)), value, swap(value, "gx", pairs_second(count_x))]
    )
    return (swap(own, "gy", pairs_first(count_y)), own, swap(own, "gy", pairs_second(count_y)))


def sum_kernel(own, first, second, *outs):
    for x, out in enumerate(outs):
        for b in range(out.shape[0]):
            out[b] = own[x, b] + first[x, b]
        for c in range(3):
            for b in range(out.shape[0]):
                out[b, c : c + 1] += second[x, c, b : b + 1]


def row_sums(own, first, second):
    return pl.pallas_call(
        sum_kernel,
        out_shape=[jax.ShapeDtypeStruct(own.shape[1:], jnp.float32)] * 3,
        in_specs=[vmem()] * 3,
        out_specs=[vmem()] * 3,
        compiler_params=pltpu.CompilerParams(vmem_limit_bytes=VMEM_LIMIT),
        name="row_sums",
    )(own, first, second)


def sent_home(first, own, second):
    count_x, count_y = lax.axis_size("gx"), lax.axis_size("gy")
    row = row_sums(
        own, swap(first, "gy", pairs_first(count_y)), swap(second, "gy", pairs_second(count_y))
    )
    return [
        row[1], swap(row[0], "gx", pairs_first(count_x)), swap(row[2], "gx", pairs_second(count_x))
    ]


def piece_of(offset, odd):
    return jnp.where(offset == 1, 1, jnp.where(offset == 2 * odd, 2, 0))


def vmem():
    return pl.BlockSpec(memory_space=pltpu.VMEM)


def smem():
    return pl.BlockSpec(memory_space=pltpu.SMEM)


def exact_parts(value):
    high = value.astype(jnp.bfloat16).astype(jnp.float32)
    rest = value - high
    middle = rest.astype(jnp.bfloat16).astype(jnp.float32)
    return high, middle, rest - middle


def pair_kernel(
    length_x,
    length_y,
    unroll,
    late,
    tower_list,
    plate_list,
    count,
    spot,
    sigma_table,
    epsilon_table,
    *refs,
):
    count_rows = 1 if late else 2
    tower_refs, plate_rows_held, refs = refs[0:4], refs[4 : 4 + count_rows], refs[4 + count_rows :]
    masks, refs = refs[0], refs[1:]
    if late:
        earlier, refs = refs[0:4], refs[4:]
    tower_outs, row_outs, held = refs[0:4], refs[4 : 4 + count_rows], refs[4 + count_rows : -1]
    listed_slots = refs[-1]
    blocks = tower_outs[0].shape[0]
    for z, ref in enumerate(tower_outs):
        ref[...] = earlier[z][...] if late else jnp.zeros_like(ref)
    for ref in row_outs:
        ref[...] = jnp.zeros_like(ref)
    odd_x, odd_y, me_z = (spot[n] for n in range(3))
    f32 = jnp.float32
    row4 = lax.broadcasted_iota(jnp.int32, (4, lanes), 0)
    lane4 = lax.broadcasted_iota(jnp.int32, (4, lanes), 1)
    sub = lax.broadcasted_iota(jnp.int32, (8, lanes), 0)
    lane = lax.broadcasted_iota(jnp.int32, (8, lanes), 1)
    lane_group = lane // 8
    on_diagonal = sub == lane % 8
    bit = jnp.left_shift(jnp.int32(1), sub)
    scale = jnp.where(
        row4 == 0,
        1.0 / length_x,
        jnp.where(row4 == 1, 1.0 / length_y, jnp.where(row4 == 2, 1.0 / length_x, 1.0)),
    ).astype(f32)
    ratio = (length_y / length_x) ** 2
    unit_sq = length_x * length_x
    soft = soft_core / unit_sq
    fall = unit_sq / cutoff_sq
    tower_scale = jnp.where(row4 == 3, coulomb_k / length_x, scale).astype(f32)
    back = jnp.where(
        row4 == 0,
        length_x / unit_sq,
        jnp.where(row4 == 1, length_y / unit_sq, length_x / unit_sq),
    ).astype(f32)
    pick = jnp.concatenate(
        [
            jnp.where(
                jnp.logical_and(
                    lax.broadcasted_iota(jnp.int32, (16, lanes), 0) % 4 == c,
                    lax.broadcasted_iota(jnp.int32, (16, lanes), 0) < 12,
                ),
                1.0,
                0.0,
            ).astype(f32)
            for c in range(4)
        ],
        axis=1,
    ).astype(jnp.bfloat16)
    all_slots = count[0]
    sigmas = [jnp.full((1, 1), sigma_table[n]) for n in range(sigma_table.shape[0])]
    depths = [jnp.sqrt(jnp.full((1, 1), epsilon_table[n])) for n in range(sigma_table.shape[0])]

    def of_kind(table, kind):
        value = table[0]
        for n in range(1, len(table)):
            value = jnp.where(kind == n, table[n], value)
        return value


    shift = blocks.bit_length() - 1

    def place(slot):
        tower, plate = tower_list[0, slot], plate_list[0, slot]
        cell = jnp.right_shift(plate, shift)
        cell_x = jnp.right_shift(cell * 11, 5)
        return (
            jnp.bitwise_xor(jnp.right_shift(tower, shift), me_z),
            jnp.bitwise_and(tower, blocks - 1),
            piece_of(cell_x, odd_x),
            piece_of(cell - 3 * cell_x, odd_y),
            jnp.bitwise_and(plate, blocks - 1),
        )

    def tower_tile(layer, row):
        near = jnp.where(layer == 0, tower_refs[0][row], tower_refs[1][row])
        return jnp.where(
            layer < 2, near, jnp.where(layer == 2, tower_refs[2][row], tower_refs[3][row])
        )

    spare = listed_slots.shape[0]
    late_row = 2 * odd_y

    def gather(step, found):
        for u in range(8):
            slot = 8 * step + u
            cell = jnp.right_shift(plate_list[0, slot], shift)
            is_late = (cell - 3 * jnp.right_shift(cell * 11, 5) == late_row).astype(jnp.int32)
            listed_slots[found] = slot
            found = found + jnp.where(slot < all_slots, is_late if late else 1 - is_late, 0)
        return found

    total = lax.fori_loop(0, tower_list.shape[1] // 8, gather, 0)

    def slot_at(number):
        slot = listed_slots[jnp.minimum(number, spare - 1)]
        return jnp.where(number < total, slot, 0)


    def prepare(slot, buffer, u):
        spread_ref, terms_ref = buffer
        layer, tower_block, cell_x, cell_y, plate_block = place(slot_at(slot))
        tower_kind = tower_tile(layer, blocks)

        def chosen(row):
            found = [ref[cell_x, row] for ref in plate_rows_held]
            return found[0] if late else jnp.where(cell_y == 0, found[0], found[1])

        plate_rows = chosen(plate_block) * scale
        plate_kind = chosen(blocks)
        of_tower = jnp.sum(
            jnp.where(lane4 == tower_block, tower_kind, 0.0), axis=1, keepdims=True
        )
        of_plate = jnp.sum(
            jnp.where(lane4 == plate_block, plate_kind, 0.0), axis=1, keepdims=True
        )
        kind_one, kind_two = of_tower[0:1], of_plate[0:1]
        sigma = 0.5 * (of_kind(sigmas, kind_one) + of_kind(sigmas, kind_two))
        depth = of_kind(depths, kind_one) * of_kind(depths, kind_two)
        sigma_sq = sigma * sigma * (1.0 / unit_sq)
        sigma_six = sigma_sq * sigma_sq * sigma_sq
        low = jnp.broadcast_to(6.0 * depth * sigma_six, (8, lanes))
        high = jnp.broadcast_to(12.0 * depth * sigma_six * sigma_six, (8, lanes))
        parts = jnp.concatenate([*exact_parts(plate_rows), jnp.zeros_like(plate_rows)], axis=0)
        spread_ref[u] = lax.dot_general(
            parts.astype(jnp.bfloat16),
            pick,
            (((0,), (0,)), ((), ())),
            preferred_element_type=f32,
        )
        terms_ref[u, 0] = low
        terms_ref[u, 1] = high

    def evaluate(slot, buffer, u):
        spread_ref, terms_ref = buffer
        layer, tower_block, cell_x, cell_y, plate_block = place(slot_at(slot))
        tower_rows = tower_tile(layer, tower_block) * tower_scale
        low, high = terms_ref[u, 0], terms_ref[u, 1]
        rows = [jnp.broadcast_to(tower_rows[c : c + 1], (8, lanes)) for c in range(4)]
        words = masks[slot_at(slot)]
        on_tower = [jnp.zeros((8, lanes), f32) for _ in range(3)]
        on_plate = [jnp.zeros((8, lanes), f32) for _ in range(3)]
        for w in range(lanes // 8):
            piece = [
                spread_ref[u, 8 * w : 8 * w + 8, lanes * c : lanes * c + lanes]
                for c in range(4)
            ]
            raw_x, raw_y, dz = (rows[c] - piece[c] for c in range(3))
            dx = raw_x - jnp.round(raw_x)
            dy = raw_y - jnp.round(raw_y)
            dist = dx * dx + ratio * (dy * dy) + dz * dz
            root = lax.rsqrt(dist + soft)
            inverse = root * root
            cube = inverse * inverse * inverse
            falloff = 1.0 - fall * dist
            word = jnp.broadcast_to(words[w : w + 1], (8, lanes))
            falloff = jnp.where(jnp.bitwise_and(word, bit) == 0, falloff, 0.0)
            falloff = jnp.maximum(falloff, 0.0) * root
            energy = cube * (high * cube - low) + rows[3] * piece[3] * root
            strength = energy * (falloff * falloff)
            for c, offset in enumerate((dx, dy, dz)):
                weighted = strength * offset
                on_tower[c] += weighted
                on_plate[c] = jnp.where(
                    lane_group == w, jnp.sum(weighted, axis=1, keepdims=True), on_plate[c]
                )
        listed = jnp.where(slot < total, 1.0, 0.0).astype(f32)
        zero = jnp.zeros((1, lanes), f32)
        tower_sum = jnp.concatenate(
            [*(jnp.sum(v, axis=0, keepdims=True) for v in on_tower), zero], axis=0
        )
        plate_sum = jnp.concatenate(
            [
                *(
                    jnp.sum(jnp.where(on_diagonal, v, 0.0), axis=0, keepdims=True)
                    for v in on_plate
                ),
                zero,
            ],
            axis=0,
        )
        factor = back * listed
        return (
            (layer, tower_block, tower_sum * factor),
            (cell_x, cell_y, plate_block, plate_sum * -factor),
        )

    def finish(done):
        for (layer, tower_block, on_tower), (cell_x, cell_y, plate_block, on_plate) in done:
            for z, ref in enumerate(tower_outs):
                ref[tower_block] += jnp.where(layer == z, on_tower, 0.0)
            for y, ref in enumerate(row_outs):
                if late:
                    place_in = pl.ds(plate_block, 1)
                    for c in range(3):
                        ref[cell_x, c, place_in, :] += on_plate[c : c + 1]
                else:
                    ref[cell_x, plate_block] += jnp.where(cell_y == y, on_plate, 0.0)

    buffers = (held[0:2], held[2:4])

    def step(index, carry):
        done = []
        for half in range(2):
            first = (2 * index + half) * unroll
            for u in range(unroll):
                prepare(first + unroll + u, buffers[1 - half], u)
                done.append(evaluate(first + u, buffers[half], u))
        finish(done)
        return carry

    for u in range(unroll):
        prepare(u, buffers[0], u)
    lax.fori_loop(0, (total + 2 * unroll - 1) // (2 * unroll), step, 0)


def pair_forces(lists, spot, tables, towers, rows, masks, lengths, earlier=()):
    late = len(earlier) > 0
    blocks = towers[0].shape[0] - 1
    slots = lists[0].shape[1]
    shape_one = jax.ShapeDtypeStruct((blocks, 4, lanes), jnp.float32)
    dims_row = (3, 3, blocks, lanes) if late else (3, blocks, 4, lanes)
    shape_row = jax.ShapeDtypeStruct(dims_row, jnp.float32)
    flops = 20 * slots * lanes * lanes
    size = 2 if late else group
    return pl.pallas_call(
        functools.partial(pair_kernel, *lengths, size, late),
        out_shape=[shape_one] * 4 + [shape_row] * len(rows),
        in_specs=[smem()] * 6 + [vmem()] * (5 + len(rows) + len(earlier)),
        out_specs=[vmem()] * (4 + len(rows)),
        scratch_shapes=[
            pltpu.VMEM((size, lanes, 4 * lanes), jnp.float32),
            pltpu.VMEM((size, 2, 8, lanes), jnp.float32),
        ]
        * 2
        + [pltpu.SMEM((slots + 1,), jnp.int32)],
        compiler_params=pltpu.CompilerParams(vmem_limit_bytes=VMEM_LIMIT),
        cost_estimate=pl.CostEstimate(
            flops=flops, bytes_accessed=2**20, transcendentals=flops // 40
        ),
        name="pairs_late" if late else "pairs_early",
    )(*lists, spot, *tables, *towers, *rows, masks, *earlier)


def arrival_kernel(spot, *refs):
    first_row, own_row, second_row, out = refs
    odd_x, odd_y = spot[0], spot[1]
    for q in range(own_row.shape[1]):
        second = [second_row[k, q] for k in range(3)]
        first = [first_row[k, q] for k in range(3)]
        own = [own_row[k, q] for k in range(3)]
        for number, (x, y) in enumerate(sources):
            wanted = float((2 - x) * 3 + (2 - y))
            by_y = own
            if y != 1:
                flip = odd_y == (1 if y == 0 else 0)
                by_y = [jnp.where(flip, first[k], second[k]) for k in range(3)]
            state = by_y[1]
            if x != 1:
                flip = odd_x == (1 if x == 0 else 0)
                state = jnp.where(flip, by_y[0], by_y[2])
            kept = jnp.where(state[6:7] == wanted, state, 0.0)
            for c in range(6):
                out[c, number : number + 1, lanes * q : lanes * q + lanes] = kept[c : c + 1]


def arrivals_of(spot, rows):
    leaving = rows[0].shape[1]
    return pl.pallas_call(
        arrival_kernel,
        out_shape=jax.ShapeDtypeStruct((6, 8, leaving * lanes), jnp.float32),
        in_specs=[smem()] + [vmem()] * 3,
        out_specs=vmem(),
        compiler_params=pltpu.CompilerParams(vmem_limit_bytes=VMEM_LIMIT),
        name="arrivals",
    )(spot, *rows)


def by_block(rows):
    return rows.reshape(rows.shape[0], -1, lanes).transpose(1, 0, 2)


def by_atom(tiles):
    return tiles.transpose(1, 0, 2).reshape(tiles.shape[1], -1)


def kick_kernel(spot, features, half_kick, inv_mass, *refs):
    parts, (positions, velocities, forces, state) = refs[:-4], refs[-4:]
    count = state.shape[0]
    leaving = [spot[3 + q] for q in range(count)]
    heading = [spot[3 + count + q] for q in range(count)]
    blocks = half_kick.shape[0]
    for b in range(blocks):
        total = parts[0][b]
        for part in parts[1:]:
            total = total + part[b]
        force = total[0:3]
        forces[b] = force
        velocities[b] = half_kick[b] + 0.5 * time_step * force * inv_mass[b : b + 1]
        positions[b] = features[b, 0:3]
    for q in range(count):
        block = leaving[q]
        state[q, 0:3] = features[block, 0:3]
        state[q, 3:6] = velocities[block]
        state[q, 6:8] = jnp.full((2, lanes), heading[q].astype(jnp.float32))
    nothing = jnp.zeros((3, lanes), jnp.float32)
    for q in range(count):
        positions[leaving[q]] = nothing
        velocities[leaving[q]] = nothing


def kick(spot, count, features, half_kick, inv_mass, parts):
    blocks = half_kick.shape[0]
    shape = jax.ShapeDtypeStruct((blocks, 3, lanes), jnp.float32)
    return pl.pallas_call(
        kick_kernel,
        out_shape=[shape] * 3
        + [jax.ShapeDtypeStruct((count, 8, lanes), jnp.float32)],
        in_specs=[smem()] + [vmem()] * (3 + len(parts)),
        out_specs=[vmem()] * 4,
        compiler_params=pltpu.CompilerParams(vmem_limit_bytes=VMEM_LIMIT),
        name="kick",
    )(spot, features, half_kick, inv_mass.reshape(blocks, lanes), *parts)


def local(
    positions,
    velocities,
    forces_old,
    inv_mass,
    charges,
    block_species,
    sigma_table,
    epsilon_table,
    tower_index,
    plate_index,
    tile_counts,
    exclusions,
    mig_block,
    mig_dest,
):
    layers = lax.axis_size("gz")
    length_x = float(lax.axis_size("gx"))
    length_y = float(lax.axis_size("gy"))
    inverse = inv_mass.reshape(-1, 1, lanes)
    half_kick = by_block(velocities) + 0.5 * time_step * by_block(forces_old) * inverse
    moved = by_block(positions) + time_step * half_kick
    kinds = block_species.astype(jnp.float32)
    kind_tile = jnp.pad(kinds[None, :], ((0, 3), (0, lanes - kinds.shape[0])))
    tiles = jnp.concatenate([moved, charges.reshape(-1, 1, lanes)], axis=1)
    features = jnp.concatenate([tiles, kind_tile[None]])
    me_x, me_y, me_z = (lax.axis_index(axis) for axis in ("gx", "gy", "gz"))
    spot = jnp.stack([me_x % 2, me_y % 2, me_z]).astype(jnp.int32)
    spot = jnp.concatenate([spot, mig_block[0], mig_dest[0]])
    rows = halo(features)

    def from_layer(value, step):
        return lax.ppermute(value, "gz", [(i, i ^ step) for i in range(layers)])

    towers = [features] + [from_layer(features, step) for step in range(1, layers)]
    first, own, second = rows

    def pairs(rows, earlier=()):
        return pair_forces(
            (tower_index, plate_index, tile_counts),
            spot,
            (sigma_table, epsilon_table),
            towers,
            rows,
            exclusions[0],
            (length_x, length_y),
            earlier,
        )

    *early, on_first, on_own = pairs((first, own))
    *sums, on_second = pairs((second,), early)
    parts = [sums[0]] + [from_layer(sums[step], step) for step in range(1, layers)]
    parts += sent_home(on_first, on_own, on_second)
    positions_new, velocities_new, forces_new, state = kick(
        spot, mig_block.shape[1], features, half_kick, inv_mass, parts
    )
    arrivals = arrivals_of(spot, halo(state))[:, None]
    return (by_atom(positions_new), by_atom(velocities_new), by_atom(forces_new), arrivals)


def solution(mesh):
    everywhere = ("gx", "gy", "gz")
    in_specs = (
        P(None, everywhere),
        P(None, everywhere),
        P(None, everywhere),
        P(everywhere),
        P(everywhere),
        P(everywhere),
        P(),
        P(),
        P(everywhere, None),
        P(everywhere, None),
        P(everywhere),
        P(everywhere, None, None, None),
        P(everywhere, None),
        P(everywhere, None),
    )
    out_specs = (
        P(None, everywhere),
        P(None, everywhere),
        P(None, everywhere),
        P(None, everywhere, None, None),
    )
    return jax.shard_map(local, mesh=mesh, in_specs=in_specs, out_specs=out_specs, check_vma=False)
```
